128 devices in a mesh: dp: 32 (over x, y, z_lo), seq: 4 (over z_hi, core).
Axes of the slice: x: 4, y: 4, z: 4 (z_hi: 2, z_lo: 2; z = z_hi * 2 + z_lo), core: 2. Of those that a mesh axis runs over, the one named last changes fastest.
Arguments:
- qkv: bfloat16 [64, 1024, 4608], P('dp', 'seq'), may hold values from -20.4 to 20.4
- gate: float32 [64, 3072], P('dp'), may hold values from 0.5 to 2.5
- cotangent: bfloat16 [64, 1024, 3072], P('dp', 'seq'), may hold values from -6 to 6
- out_weight: bfloat16 [1536, 3072], replicated, may hold values from -0.15625 to 0.15625
- clip_lengths: int32 [64], replicated, may hold values from 1 to 768, as said below
- text_lengths: int32 [64], replicated, may hold values from 1 to 256, as said below
- plan: int32 [32], replicated, may hold values from 0 to 31, as said below
Outputs:
- mixed: bfloat16 [64, 1024, 3072], P('dp', 'seq')
- gate_grad: float32 [64, 3072], P('dp')
- weight_grad: float32 [1536, 3072], P(None, ('dp', 'seq'))
- qkv_grad: bfloat16 [64, 1024, 4608], P('dp', 'seq')
The draws below stay inside these ranges and needn't reach their ends.
Inputs may be any that keep to these rules, and one draw needn't show every extreme that they name: clip_lengths[c] counts the live video positions of source clip c = 2 g + s (group g, slot s); some clip has exactly 768. text_lengths[c] counts the live text positions of source clip c; some clip has exactly 256. plan is a permutation of 0 to 31: the second clip of group g becomes the second clip of group plan[g].
All inputs are finite; a program needn't handle non-finite values.
Results may differ from the reference program's by a relative error of at most 0.011.
Values may be sent and summed in bfloat16 or wider, within the bound.
No kernel may reach another device: no remote copies, remote signals or barrier semaphores. Data moves between devices by JAX's collectives and lax.ppermute only.
A program may use at most 128 MiB of HBM per device.

```python
import jax
import jax.numpy as jnp
from jax import lax

D = 3072
HEADS = 12
HD = 128
TXT = 256
CLIP = 768
GROUPS = 32
CLIPS = 64
SEQ = 1024


def draw_qkv(key, part):
    head_width = HEADS * HD
    full_width = 3 * head_width
    normal_draw = jnp.clip(jax.random.normal(key, (CLIPS, SEQ, full_width), jnp.float32), -6.0, 6.0)
    return normal_draw.astype(jnp.bfloat16)


def length_table(key):
    folded = jax.random.fold_in(key, 11)
    k_heavy, k_long, k_short, k_peak = jax.random.split(folded, 4)
    heavier = jax.random.randint(k_heavy, (GROUPS, 1), 0, 2)
    longer = jax.random.randint(k_long, (GROUPS, 2), CLIP // 2 + 1, CLIP + 1)
    shorter = jax.random.randint(k_short, (GROUPS, 2), 1, CLIP // 4 + 1)
    lengths_all = jnp.where(heavier == 1, longer, shorter).reshape(CLIPS)
    peak_index = jax.random.randint(k_peak, (), 0, CLIPS)
    return jnp.where(jnp.arange(CLIPS) == peak_index, CLIP, lengths_all).astype(jnp.int32)


def draw_clip_lengths(key, part):
    return length_table(key)


def draw_plan(key, part):
    lengths_all = length_table(key)
    ordinal = jnp.arange(GROUPS, dtype=jnp.int32)
    first_keys = lengths_all[0::2] * GROUPS + ordinal
    second = lengths_all[1::2] * GROUPS + ordinal
    longest = jnp.argsort(-first_keys, stable=True).astype(jnp.int32)
    shortest = jnp.argsort(second, stable=True).astype(jnp.int32)
    return jnp.zeros((GROUPS,), jnp.int32).at[shortest].set(longest)


def draw_text_lengths(key, part):
    folded = jax.random.fold_in(key, 23)
    k_draw, k_peak = jax.random.split(folded, 2)
    lengths_all = jax.random.randint(k_draw, (CLIPS,), 1, TXT + 1)
    peak_index = jax.random.randint(k_peak, (), 0, CLIPS)
    return jnp.where(jnp.arange(CLIPS) == peak_index, TXT, lengths_all).astype(jnp.int32)


def level_of(key, shape, shards, low, top_value):
    def one(position, blocks):
        heights = jax.random.uniform(jax.random.fold_in(jax.random.fold_in(key, 6), position), (blocks,), jnp.float32, low / len(shards), top_value / len(shards))
        return jnp.repeat(jnp.exp(heights), shape[position] // blocks).reshape((-1,) + (1,) * (len(shape) - position - 1))

    gain = one(*shards[0])
    for cut in shards[1:]:
        gain = gain * one(*cut)
    return gain


def bell_draw(stream_key, dims, spread, limit, cuts=(), kind=jnp.bfloat16):
    drawn = jax.random.normal(stream_key, dims, jnp.float32) * spread
    if len(cuts) > 0:
        drawn = level_of(stream_key, dims, cuts, -0.22, 0.18) * drawn
    return jnp.clip(drawn, min=-limit, max=limit).astype(kind)


def setup_inputs(seed: int = 0) -> dict:
    streams_of = jax.random.split(jax.random.key(seed), 8)
    qkv = draw_qkv(jax.random.fold_in(streams_of[7], 71), 0)
    gate = jnp.clip(0.5 + 2.0 * jax.random.uniform(streams_of[1], (CLIPS, D), jnp.float32) ** level_of(streams_of[1], (CLIPS, D), ((0, 32),), -0.2, 0.2), 0.5, 2.5)
    cotangent = bell_draw(streams_of[2], (CLIPS, SEQ, D), 1.0, 6.0, ((0, 32), (1, 4)))
    out_weight = bell_draw(streams_of[3], (HEADS * HD, D), (HEADS * HD) ** -0.5, 0.15625)
    clip_lengths = draw_clip_lengths(jax.random.fold_in(streams_of[7], 71), 0)
    text_lengths = draw_text_lengths(jax.random.fold_in(streams_of[7], 71), 0)
    plan = draw_plan(jax.random.fold_in(streams_of[7], 71), 0)
    return {"qkv": qkv, "gate": gate, "cotangent": cotangent, "out_weight": out_weight, "clip_lengths": clip_lengths, "text_lengths": text_lengths, "plan": plan}


NEGATIVE = -1e30


def allowed_rows(text_len, video_len):
    places = jnp.arange(SEQ, dtype=jnp.int32)
    return (places < text_len) | ((places >= TXT) & (places < TXT + video_len))


def reference(qkv, gate, cotangent, out_weight, clip_lengths, text_lengths, plan):
    head_width = HEADS * HD
    ordinal = jnp.arange(GROUPS, dtype=jnp.int32)
    inverse = jnp.zeros((GROUPS,), jnp.int32).at[plan].set(ordinal)
    source_of = jnp.stack([2 * ordinal, 2 * inverse + 1], axis=1).reshape(CLIPS).astype(jnp.int32)
    score_scale = HD ** -0.5

    def clip_step(weight_sum, inputs):
        tokens, gate_row, grad_row, text_len, video_len = inputs
        allowed = allowed_rows(text_len, video_len)
        live_pairs = (allowed[:, None] & allowed[None, :])[None]
        queries = tokens[:, :head_width].reshape(SEQ, HEADS, HD).astype(jnp.float32)
        keys_all = tokens[:, head_width:2 * head_width].reshape(SEQ, HEADS, HD).astype(jnp.float32)
        values_all = tokens[:, 2 * head_width:].reshape(SEQ, HEADS, HD).astype(jnp.float32)
        scores = jnp.einsum('qhd,khd->hqk', queries, keys_all) * score_scale
        masked = jnp.where(live_pairs, scores, NEGATIVE)
        row_peak = jnp.max(masked, axis=-1, keepdims=True)
        row_total = jnp.sum(jnp.exp(masked - row_peak), axis=-1, keepdims=True)
        log_total = row_peak + jnp.log(row_total)
        probabilities = jnp.exp(jnp.where(live_pairs, scores - log_total, NEGATIVE))
        probs_low = lax.optimization_barrier(probabilities.astype(jnp.bfloat16))
        attended = jnp.einsum('hqk,khd->qhd', probs_low.astype(jnp.float32), values_all).astype(jnp.bfloat16)
        attended = lax.optimization_barrier(attended)
        attended_flat = attended.reshape(SEQ, head_width)
        outputs = jnp.dot(attended_flat, out_weight, preferred_element_type=jnp.float32)
        mixed = (gate_row[None, :] * outputs).astype(jnp.bfloat16)
        gate_grad = jnp.sum(grad_row.astype(jnp.float32) * outputs, axis=0)
        scaled = (grad_row.astype(jnp.float32) * gate_row[None, :]).astype(jnp.bfloat16)
        weight_sum = weight_sum + jnp.dot(attended_flat.T, scaled, preferred_element_type=jnp.float32)
        d_attn = jnp.dot(scaled, out_weight.T, preferred_element_type=jnp.float32).astype(jnp.bfloat16)
        d_attn = lax.optimization_barrier(d_attn)
        d_heads = d_attn.reshape(SEQ, HEADS, HD).astype(jnp.float32)
        row_dots = jnp.einsum('qhd,qhd->hq', d_heads, attended.astype(jnp.float32))
        d_probs = jnp.einsum('qhd,khd->hqk', d_heads, values_all)
        d_scores = lax.optimization_barrier((probabilities * (d_probs - row_dots[..., None])).astype(jnp.bfloat16))
        d_scores = d_scores.astype(jnp.float32)
        grad_q = jnp.einsum('hqk,khd->qhd', d_scores, keys_all) * score_scale
        grad_k = jnp.einsum('hqk,qhd->khd', d_scores, queries) * score_scale
        grad_v = jnp.einsum('hqk,qhd->khd', probs_low.astype(jnp.float32), d_heads)
        gradients = jnp.concatenate([grad_q.reshape(SEQ, head_width), grad_k.reshape(SEQ, head_width), grad_v.reshape(SEQ, head_width)], axis=1).astype(jnp.bfloat16)
        return weight_sum, (mixed, gate_grad, gradients)

    scan_inputs = (qkv[source_of], gate, cotangent, text_lengths[source_of], clip_lengths[source_of])
    weight_grad, (mixed, gate_grad, balanced_grads) = lax.scan(clip_step, jnp.zeros((head_width, D), jnp.float32), scan_inputs)
    qkv_grad = jnp.zeros_like(qkv).at[source_of].set(balanced_grads)
    return mixed, gate_grad, weight_grad, qkv_grad
```

```python
import functools

import jax
import jax.numpy as jnp
from jax import lax
from jax.experimental import pallas as pl
from jax.experimental.pallas import tpu as pltpu
from jax.sharding import PartitionSpec as P


HD = 128
ROWS = 256
HEADS_HALF = 6
HALF = HEADS_HALF * HD
WIDTH = 2 * HALF
TOGETHER = 2
D = 3072
NEGATIVE = -1e30
LOG2E = 1.4426950408889634
SCALE = HD**-0.5

NT = (((1,), (1,)), ((), ()))
NN = (((1,), (0,)), ((), ()))
TN = (((0,), (0,)), ((), ()))


def mm(a, b, dims):
    return lax.dot_general(a, b, dims, preferred_element_type=jnp.float32)


def cost(flops, nbytes, transcendentals=0):
    return pl.CostEstimate(
        flops=int(flops), bytes_accessed=int(nbytes), transcendentals=int(transcendentals)
    )


def swap(x, step):
    return lax.ppermute(x, "seq", [(i, i ^ step) for i in range(4)])


def prep_kernel(sp, qo, ko, vo, kc, vc, s1, s2, s3):
    s1[0] = qo[0]
    s1[1] = ko[0]
    s1[2] = vo[0]
    s2[0] = kc[0]
    s2[1] = vc[0]
    s3[0] = ko[0]
    s3[1] = vo[0]


def prep(sp, qkv, slot):
    rows = ROWS // 2

    def half(member, other):
        def index(r, sp):
            core = sp[0, 0]
            return (slot, r, 2 * member + (1 - core if other else core))

        return pl.BlockSpec((1, rows, HALF), index)

    def out(count):
        return pl.BlockSpec((count, rows, HALF), lambda r, sp: (0, r, 0))

    def shape(count):
        return jax.ShapeDtypeStruct((count, ROWS, HALF), jnp.bfloat16)

    return pl.pallas_call(
        prep_kernel,
        grid_spec=pltpu.PrefetchScalarGridSpec(
            num_scalar_prefetch=1,
            grid=(2,),
            in_specs=[half(0, True), half(1, True), half(2, True), half(1, False), half(2, False)],
            out_specs=[out(3), out(2), out(2)],
        ),
        out_shape=[shape(3), shape(2), shape(2)],
        cost_estimate=cost(1e6, 5e6),
    )(sp, qkv, qkv, qkv, qkv, qkv)


def live_limit(sp, slot, block, shape, axis):
    return lax.broadcasted_iota(jnp.int32, shape, axis) < sp[slot, 1 + block]


def key_bias(sp, slot, axis):
    shape = (ROWS, 1) if axis == 0 else (1, ROWS)
    parts = [
        jnp.where(live_limit(sp, slot, block, shape, axis), 0.0, NEGATIVE) for block in range(4)
    ]
    return jnp.concatenate(parts, axis=axis)


def fwd_kernel(slot, sp, q0, k0, v0, q1, k1, v1, k2, v2, k3, v3, att, lse):
    bias = key_bias(sp, slot, 1)
    work = []
    for head in range(TOGETHER):
        cols = slice(head * HD, (head + 1) * HD)
        keys = jnp.concatenate([k[0, :, cols] for k in (k0, k1, k2, k3)], axis=0)
        values = jnp.concatenate([v[0, :, cols] for v in (v0, v1, v2, v3)], axis=0)
        for block, q in enumerate((q0, q1)):
            work.append((head, cols, block, mm(q[0, :, cols], keys, NT), values))
    for head, cols, block, products, values in work:
        scores = products * (SCALE * LOG2E) + bias
        peak = jnp.max(scores, axis=1, keepdims=True)
        powers = jnp.exp2(scores - peak)
        total = jnp.sum(powers, axis=1, keepdims=True)
        live = live_limit(sp, slot, block, (ROWS, 1), 0)
        inverse = jnp.where(live, 1.0 / total, 0.0)
        mixed = mm(powers.astype(jnp.bfloat16), values, NN) * inverse
        att[block, :, cols] = mixed.astype(jnp.bfloat16)
        level = jnp.where(live, peak + jnp.log2(total), -NEGATIVE)
        lse[head, :, block * ROWS : (block + 1) * ROWS] = jnp.broadcast_to(level, (ROWS, HD)).T[:8]


def bwd_kernel(
    slot, sp, q0, k0, v0, q1, k1, v1, k2, v2, k3, v3, att, lse, do0, do1, own, r1, r2, r3
):
    keys = jnp.concatenate([k0[0], k1[0], k2[0], k3[0]], axis=0)
    values = jnp.concatenate([v0[0], v1[0], v2[0], v3[0]], axis=0)
    bias = key_bias(sp, slot, 0)
    grad_k = None
    grad_v = None
    for block, (q, do) in enumerate(((q0, do0), (q1, do1))):
        d_rows = do[0]
        scores = mm(keys, q[0], NT) * (SCALE * LOG2E) + bias
        level = lse[0, 0:1, block * ROWS : (block + 1) * ROWS]
        probs = jnp.exp2(scores - level)
        product = d_rows.astype(jnp.float32) * att[block].astype(jnp.float32)
        dots = jnp.sum(product.T, axis=0, keepdims=True)
        d_probs = mm(values, d_rows, NT)
        d_scores = (probs * (d_probs - dots)).astype(jnp.bfloat16)
        v_part = mm(probs.astype(jnp.bfloat16), d_rows, NN)
        k_part = mm(d_scores, q[0], NN)
        grad_k = k_part if block == 0 else grad_k + k_part
        grad_v = v_part if block == 0 else grad_v + v_part
        grad_q = (mm(keys, d_scores, TN) * SCALE).T
        if block == 0:
            own[0] = grad_q
        else:
            r1[0] = grad_q.astype(jnp.bfloat16)
    grad_k = grad_k * SCALE
    own[1] = grad_k[:ROWS]
    own[2] = grad_v[:ROWS]
    r1[1] = grad_k[ROWS : 2 * ROWS].astype(jnp.bfloat16)
    r1[2] = grad_v[ROWS : 2 * ROWS].astype(jnp.bfloat16)
    r2[0] = grad_k[2 * ROWS : 3 * ROWS].astype(jnp.bfloat16)
    r2[1] = grad_v[2 * ROWS : 3 * ROWS].astype(jnp.bfloat16)
    r3[0] = grad_k[3 * ROWS :].astype(jnp.bfloat16)
    r3[1] = grad_v[3 * ROWS :].astype(jnp.bfloat16)


def head_block(lead, index=0, heads=1):
    return pl.BlockSpec((lead, ROWS, heads * HD), lambda h, sp: (index, 0, h))


def section_specs(slot, heads=1):
    def own(member):
        return pl.BlockSpec(
            (1, ROWS, heads * HD),
            lambda h, sp: (slot, 0, (12 * member + HEADS_HALF * sp[0, 0]) // heads + h),
        )

    return [own(0), own(1), own(2)] + [head_block(1, m, heads) for m in (0, 1, 2, 0, 1, 0, 1)]


def sections(qkv, x1, x2, x3):
    return (qkv, qkv, qkv, x1, x1, x1, x2, x2, x3, x3)


LSE_SPEC = pl.BlockSpec((1, 8, 2 * ROWS), lambda h, sp: (h, 0, 0))
PAIRS = HEADS_HALF * 512 * 1024


def attend(sp, slot, qkv, received):
    return pl.pallas_call(
        functools.partial(fwd_kernel, slot),
        grid_spec=pltpu.PrefetchScalarGridSpec(
            num_scalar_prefetch=1,
            grid=(HEADS_HALF // TOGETHER,),
            in_specs=section_specs(slot, TOGETHER),
            out_specs=[
                head_block(2, 0, TOGETHER),
                pl.BlockSpec((TOGETHER, 8, 2 * ROWS), lambda h, sp: (h, 0, 0)),
            ],
        ),
        out_shape=[
            jax.ShapeDtypeStruct((2, ROWS, HALF), jnp.bfloat16),
            jax.ShapeDtypeStruct((HEADS_HALF, 8, 2 * ROWS), jnp.float32),
        ],
        cost_estimate=cost(4 * PAIRS * HD, 5e6, PAIRS),
    )(sp, *sections(qkv, *received))


def attend_back(sp, slot, qkv, received, att, lse, d_own, d_peer):
    d_own_spec = pl.BlockSpec((1, ROWS, HD), lambda h, sp: (0, 0, HEADS_HALF * sp[0, 0] + h))

    def shape(count, kind):
        return jax.ShapeDtypeStruct((count, ROWS, HALF), kind)

    return pl.pallas_call(
        functools.partial(bwd_kernel, slot),
        grid_spec=pltpu.PrefetchScalarGridSpec(
            num_scalar_prefetch=1,
            grid=(HEADS_HALF,),
            in_specs=section_specs(slot) + [head_block(2), LSE_SPEC, d_own_spec, head_block(1)],
            out_specs=[head_block(3), head_block(3), head_block(2), head_block(2)],
        ),
        out_shape=[
            shape(3, jnp.float32),
            shape(3, jnp.bfloat16),
            shape(2, jnp.bfloat16),
            shape(2, jnp.bfloat16),
        ],
        cost_estimate=cost(10 * PAIRS * HD, 1e7, PAIRS),
    )(sp, *sections(qkv, *received), att, lse, d_own, d_peer)


def join_kernel(sp, own, p1, p2, p3, *rest):
    out = rest[-1]
    core = sp[0, 0]
    member = pl.program_id(0)
    crossing = jnp.where(member > 0, 1.0, 0.0)
    mine = own[0] + crossing * p2[0].astype(jnp.float32)
    other = p1[0].astype(jnp.float32) + crossing * p3[0].astype(jnp.float32)
    first = core == 0
    out[0, :, :HALF] = jnp.where(first, mine, other).astype(jnp.bfloat16)
    out[0, :, HALF:] = jnp.where(first, other, mine).astype(jnp.bfloat16)


def join(sp, slot, own, p1, p2, p3, base):
    def piece(shift):
        return pl.BlockSpec((1, ROWS, HALF), lambda m, sp: (jnp.maximum(m - shift, 0), 0, 0))

    in_specs = [piece(0), piece(0), piece(1), piece(1)]
    args = [own, p1, p2, p3]
    aliases = {}
    if base is not None:
        in_specs.append(pl.BlockSpec(memory_space=pl.ANY))
        args.append(base)
        aliases = {5: 0}
    return pl.pallas_call(
        join_kernel,
        grid_spec=pltpu.PrefetchScalarGridSpec(
            num_scalar_prefetch=1,
            grid=(3,),
            in_specs=in_specs,
            out_specs=pl.BlockSpec((1, ROWS, WIDTH), lambda m, sp: (slot, 0, m)),
        ),
        out_shape=jax.ShapeDtypeStruct((2, ROWS, 3 * WIDTH), jnp.bfloat16),
        input_output_aliases=aliases,
        cost_estimate=cost(1e6, 1e7),
    )(sp, *args)


def pick_kernel(order, rows, out):
    def step(slot, carry):
        out[slot] = rows[order[slot]]
        return carry

    lax.fori_loop(0, rows.shape[0], step, 0)


def pick(rows, order):
    whole = pl.BlockSpec(rows.shape, lambda i, order: (0, 0, 0))
    return pl.pallas_call(
        pick_kernel,
        grid_spec=pltpu.PrefetchScalarGridSpec(
            num_scalar_prefetch=1, grid=(1,), in_specs=[whole], out_specs=whole
        ),
        out_shape=jax.ShapeDtypeStruct(rows.shape, rows.dtype),
        cost_estimate=cost(1e6, 2 * rows.size * 2),
        name="pick",
    )(order, rows)


def rows_kernel(sp, cotangent, gate, weight, send, keep, away, near, near_send, total):
    step = pl.program_id(0)
    parts = [
        (cotangent[slot].astype(jnp.float32) * gate[slot : slot + 1]).astype(jnp.bfloat16)
        for slot in range(2)
    ]

    @pl.when(step < 3)
    def _():
        send[0] = parts[0]
        send[1] = parts[1]

    @pl.when(step >= 3)
    def _():
        keep[0] = parts[0]
        keep[1] = parts[1]

    product = mm(jnp.concatenate(parts, axis=0), weight[...], NT)

    @pl.when(step == 0)
    def _():
        total[...] = product

    @pl.when((step > 0) & (step < 5))
    def _():
        total[...] += product

    @pl.when(step == 5)
    def _():
        rows = (total[...] + product).astype(jnp.bfloat16)
        near[...] = rows[:ROWS]
        away[...] = rows[ROWS:]
        near_send[0] = jnp.where(sp[0, 0] == 0, rows[:ROWS, HALF:], rows[:ROWS, :HALF])


def scaled_rows(sp, cotangent, gate, out_weight):
    cols = D // 6

    def place(step, sp):
        core = sp[0, 0]
        return jnp.where(step < 3, 3 * (1 - core), 3 * core - 3) + step

    def whole(*shape):
        return pl.BlockSpec(shape, lambda k, sp: (0,) * len(shape))

    def shape(*dims):
        return jax.ShapeDtypeStruct(dims, jnp.bfloat16)

    return pl.pallas_call(
        rows_kernel,
        grid_spec=pltpu.PrefetchScalarGridSpec(
            num_scalar_prefetch=1,
            grid=(6,),
            in_specs=[
                pl.BlockSpec((2, ROWS, cols), lambda k, sp: (0, 0, place(k, sp))),
                pl.BlockSpec((2, cols), lambda k, sp: (0, place(k, sp))),
                pl.BlockSpec((WIDTH, cols), lambda k, sp: (0, place(k, sp))),
            ],
            out_specs=[
                pl.BlockSpec((2, ROWS, cols), lambda k, sp: (0, 0, jnp.minimum(k, 2))),
                pl.BlockSpec((2, ROWS, cols), lambda k, sp: (0, 0, jnp.maximum(k - 3, 0))),
                whole(ROWS, WIDTH),
                whole(ROWS, WIDTH),
                whole(1, ROWS, HALF),
            ],
            scratch_shapes=[pltpu.VMEM((2 * ROWS, WIDTH), jnp.float32)],
        ),
        out_shape=[
            shape(2, ROWS, D // 2),
            shape(2, ROWS, D // 2),
            shape(ROWS, WIDTH),
            shape(ROWS, WIDTH),
            shape(1, ROWS, HALF),
        ],
        cost_estimate=cost(2 * 512 * WIDTH * D, 1.7e7),
        name="scaled_rows",
    )(sp, cotangent, gate, out_weight)


def project_kernel(sp, a0, a1, b0, b1, w_mine, w_other, gate, cotangent, mixed, gate_grad):
    mine = jnp.concatenate([a0[0], a1[0]], axis=0)
    other = jnp.concatenate([b0[0], b1[0]], axis=0)
    outputs = mm(mine, w_mine[...], NN) + mm(other, w_other[...], NN)
    for slot in range(2):
        rows = outputs[slot * ROWS : (slot + 1) * ROWS]
        mixed[slot] = (rows * gate[slot : slot + 1]).astype(jnp.bfloat16)
        gate_grad[slot : slot + 1] = jnp.sum(
            cotangent[slot].astype(jnp.float32) * rows, axis=0, keepdims=True
        )


def project(sp, mine, other, out_weight, gate, cotangent):
    cols = 512

    def rows(index):
        return pl.BlockSpec((1, ROWS, HALF), lambda d, sp: (index, 0, 0))

    wide = pl.BlockSpec((2, ROWS, cols), lambda d, sp: (0, 0, d))
    thin = pl.BlockSpec((2, cols), lambda d, sp: (0, d))
    return pl.pallas_call(
        project_kernel,
        grid_spec=pltpu.PrefetchScalarGridSpec(
            num_scalar_prefetch=1,
            grid=(D // cols,),
            in_specs=[
                rows(0),
                rows(0),
                rows(1),
                rows(1),
                pl.BlockSpec((HALF, cols), lambda d, sp: (sp[0, 0], d)),
                pl.BlockSpec((HALF, cols), lambda d, sp: (1 - sp[0, 0], d)),
                thin,
                wide,
            ],
            out_specs=[wide, thin],
        ),
        out_shape=[
            jax.ShapeDtypeStruct((2, ROWS, D), jnp.bfloat16),
            jax.ShapeDtypeStruct((2, D), jnp.float32),
        ],
        cost_estimate=cost(2 * 512 * WIDTH * D, 1.6e7),
        name="project",
    )(sp, mine[0], mine[1], other[0], other[1], out_weight, out_weight, gate, cotangent)


def weigh_kernel(sp, scaled_own, scaled_peer, a0, a1, b0, b1, out):
    left = jnp.concatenate(
        [scaled_own[0], scaled_peer[0], scaled_own[1], scaled_peer[1]], axis=0
    )
    mine = jnp.concatenate([a0[0], a0[1], a1[0], a1[1]], axis=0)
    other = jnp.concatenate([b0[1], b0[0], b1[1], b1[0]], axis=0)
    first = sp[0, 0] == 0
    low = jnp.where(first, mine, other)
    high = jnp.where(first, other, mine)
    out[:, :HALF] = mm(left, low, TN).astype(jnp.bfloat16)
    out[:, HALF:] = mm(left, high, TN).astype(jnp.bfloat16)


def weigh(sp, scaled, scaled_peer, mine, other):
    rows = 384
    steps = D // 2 // rows
    pair = pl.BlockSpec((2, ROWS, HALF), lambda d, sp: (0, 0, 0))
    return pl.pallas_call(
        weigh_kernel,
        grid_spec=pltpu.PrefetchScalarGridSpec(
            num_scalar_prefetch=1,
            grid=(steps,),
            in_specs=[
                pl.BlockSpec((2, ROWS, rows), lambda d, sp: (0, 0, d)),
                pl.BlockSpec((2, ROWS, rows), lambda d, sp: (0, 0, d)),
                pair,
                pair,
                pair,
                pair,
            ],
            out_specs=pl.BlockSpec((rows, WIDTH), lambda d, sp: (d, 0)),
        ),
        out_shape=jax.ShapeDtypeStruct((D // 2, WIDTH), jnp.bfloat16),
        cost_estimate=cost(2 * 1024 * WIDTH * D // 2, 1.2e7),
        name="weigh",
    )(sp, scaled, scaled_peer, mine[0], mine[1], other[0], other[1])


def plane_groups():
    return [[2 * xy + z_low for xy in range(16)] for z_low in range(2)]


def final_moves(step):
    moves = []
    for xy in range(16):
        for z_low in range(2):
            for z_high in range(2):
                for core in range(2):
                    source = 4 * (2 * xy + z_low) + 2 * z_high + core
                    target = 4 * (16 * core + xy) + ((2 * z_low + z_high) ^ step)
                    moves.append((source, target))
    return moves


def sum_kernel(sp, spread, *rest):
    total = rest[-1]
    total[...] = jnp.sum(spread[...].astype(jnp.float32), axis=0)
    count = total.shape[0] // 4
    for step, out in enumerate(rest[:-1]):
        start = pl.multiple_of((sp[1, 0] ^ step) * count, 8)
        out[...] = total[pl.ds(start, count), :].astype(jnp.bfloat16)


def sum_weights(sp, spread):
    groups, count, _ = spread.shape
    cols = 512
    quarter = pl.BlockSpec((count // 4, cols), lambda i, sp: (0, i))
    shape = jax.ShapeDtypeStruct((count // 4, WIDTH), jnp.bfloat16)
    return pl.pallas_call(
        sum_kernel,
        grid_spec=pltpu.PrefetchScalarGridSpec(
            num_scalar_prefetch=1,
            grid=(WIDTH // cols,),
            in_specs=[pl.BlockSpec((groups, count, cols), lambda i, sp: (0, 0, i))],
            out_specs=[quarter] * 4,
            scratch_shapes=[pltpu.VMEM((count, cols), jnp.float32)],
        ),
        out_shape=[shape] * 4,
        cost_estimate=cost(5e6, 5e6),
        name="sum_weights",
    )(sp, spread)


def finish_weights(quarters):
    pieces = [
        lax.ppermute(quarter, ("dp", "seq"), final_moves(step)).astype(jnp.float32)
        for step, quarter in enumerate(quarters)
    ]
    return (pieces[0] + pieces[1] + pieces[2] + pieces[3]).T


def after(value, *others):
    return lax.optimization_barrier((value, *others))[0]


def spread_out(rows):
    groups = lax.axis_size("dp")
    portions = rows.reshape(groups, -1, rows.shape[-1])
    return lax.all_to_all(portions, "dp", split_axis=0, concat_axis=0, tiled=True)


def land(arranged, shape):
    landed = lax.all_to_all(arranged, "dp", split_axis=0, concat_axis=0, tiled=True)
    return landed.reshape(shape)


def body(qkv, gate, cotangent, out_weight, clip_lengths, text_lengths, plan):
    groups = lax.axis_size("dp")
    group_index = lax.axis_index("dp")
    seq_index = lax.axis_index("seq")
    core = seq_index & 1
    z_place = 2 * (group_index & 1) + (seq_index >> 1)
    ordinal = jnp.arange(groups, dtype=jnp.int32)
    inverse = jnp.sum(jnp.where(plan[None, :] == ordinal[:, None], ordinal[None, :], 0), axis=1)

    quarters = seq_index ^ jnp.arange(4, dtype=jnp.int32)
    text = lax.dynamic_slice_in_dim(text_lengths, 2 * group_index, 2)[:, None]
    video = lax.dynamic_slice_in_dim(clip_lengths, 2 * group_index, 2)[:, None]
    limits = jnp.where(quarters[None] == 0, text, video - (quarters[None] - 1) * ROWS)
    place = jnp.stack([core, z_place]).astype(jnp.int32)[:, None]
    sp = jnp.concatenate([place, limits.astype(jnp.int32)], axis=1)
    first = core == 0

    def to_core(rows):
        other = jnp.where(first, rows[:, HALF:], rows[:, :HALF])
        return swap(other[None], 1)

    received = [None, None]
    d_own, d_peer = [None, None], [None, None]
    att, lse = [None, None], [None, None]

    s1, s2, s3 = prep(sp, qkv, 1)
    received[1] = (swap(s1, 1), swap(s2, 2), swap(s3, 3))
    scaled_send, scaled, away, near, near_send = scaled_rows(
        after(sp, s2), cotangent, gate, out_weight
    )
    d_spread = spread_out(away)
    s1, s2, s3 = prep(after(sp, away), qkv, 0)
    received[0] = (swap(s1, 1), swap(s2, 2), swap(s3, 3))
    d_own[0], d_peer[0] = near[None], swap(near_send, 1)
    scaled_peer = swap(scaled_send, 1)

    att[1], lse[1] = attend(after(sp, s2), 1, qkv, received[1])
    att_spread = spread_out(att[1].reshape(2 * ROWS, HALF))
    d_picked = pick(d_spread, after(plan, lse[1]))
    att[0], lse[0] = attend(after(sp, d_picked), 0, qkv, received[0])
    att_other = [swap(att[0], 1)]
    picked = pick(att_spread, after(inverse, lse[0]))
    moved = land(picked, (2, ROWS, HALF))
    landed = land(after(d_picked, moved), (ROWS, WIDTH))

    def back(sp, slot):
        return attend_back(
            sp, slot, qkv, received[slot], att[slot], lse[slot], d_own[slot], d_peer[slot]
        )

    own_0, *sent_0 = back(after(sp, picked), 0)
    pieces_0 = [swap(rows, 1 + i) for i, rows in enumerate(sent_0)]
    d_own[1], d_peer[1] = landed[None], to_core(landed)
    balanced = [att[0], moved]
    att_other.append(swap(moved, 1))
    partial = weigh(after(sp, sent_0[1]), scaled, scaled_peer, balanced, att_other)
    spread = lax.all_to_all(
        partial.reshape(16, WIDTH // 16, WIDTH),
        "dp",
        split_axis=0,
        concat_axis=0,
        tiled=True,
        axis_index_groups=plane_groups(),
    )
    own_1, *sent_1 = back(after(sp, partial), 1)
    pieces_1 = [swap(rows, 1 + i) for i, rows in enumerate(sent_1)]
    mixed, gate_part = project(
        after(sp, sent_1[1]), balanced, att_other, out_weight, gate, cotangent
    )
    gate_grad = gate_part + swap(gate_part, 1) + swap(gate_part, 2) + swap(gate_part, 3)
    grads = join(after(sp, gate_part), 0, own_0, *pieces_0, None)
    quarters = sum_weights(after(sp, grads), spread)
    weight_grad = finish_weights(quarters)
    grads = join(after(sp, quarters[0]), 1, own_1, *pieces_1, grads)
    return (mixed, gate_grad, weight_grad, grads)


def solution(mesh):
    in_specs = (P("dp", "seq", None), P("dp", None), P("dp", "seq", None), P(), P(), P(), P())
    out_specs = (P("dp", "seq", None), P("dp", None), P(None, ("dp", "seq")), P("dp", "seq", None))
    return jax.shard_map(body, mesh=mesh, in_specs=in_specs, out_specs=out_specs, check_vma=False)
```

```python
import functools

import jax
import jax.numpy as jnp
from jax import lax
from jax.experimental import pallas as pl
from jax.experimental.pallas import tpu as pltpu
from jax.sharding import PartitionSpec as P


HD = 128
ROWS = 256
HEADS_HALF = 6
HALF = HEADS_HALF * HD
WIDTH = 2 * HALF
TOGETHER = 2
SHARE = 96
D = 3072
NEGATIVE = -1e30
LOG2E = 1.4426950408889634
SCALE = HD**-0.5

NT = (((1,), (1,)), ((), ()))
NN = (((1,), (0,)), ((), ()))
TN = (((0,), (0,)), ((), ()))


def mm(a, b, dims):
    return lax.dot_general(a, b, dims, preferred_element_type=jnp.float32)


def cost(flops, nbytes, transcendentals=0):
    return pl.CostEstimate(
        flops=int(flops), bytes_accessed=int(nbytes), transcendentals=int(transcendentals)
    )


def swap(x, step):
    return lax.ppermute(x, "seq", [(i, i ^ step) for i in range(4)])


def prep_kernel(sp, qo, ko, vo, kc, vc, s1, s2, s3):
    s1[0] = qo[0]
    s1[1] = ko[0]
    s1[2] = vo[0]
    s2[0] = kc[0]
    s2[1] = vc[0]
    s3[0] = ko[0]
    s3[1] = vo[0]


def prep(sp, qkv, slot):
    rows = ROWS // 2

    def half(member, other):
        def index(r, sp):
            core = sp[0, 0]
            return (slot, r, 2 * member + (1 - core if other else core))

        return pl.BlockSpec((1, rows, HALF), index)

    def out(count):
        return pl.BlockSpec((count, rows, HALF), lambda r, sp: (0, r, 0))

    def shape(count):
        return jax.ShapeDtypeStruct((count, ROWS, HALF), jnp.bfloat16)

    return pl.pallas_call(
        prep_kernel,
        grid_spec=pltpu.PrefetchScalarGridSpec(
            num_scalar_prefetch=1,
            grid=(2,),
            in_specs=[half(0, True), half(1, True), half(2, True), half(1, False), half(2, False)],
            out_specs=[out(3), out(2), out(2)],
        ),
        out_shape=[shape(3), shape(2), shape(2)],
        cost_estimate=cost(1e6, 5e6),
    )(sp, qkv, qkv, qkv, qkv, qkv)


def live_limit(sp, slot, block, shape, axis):
    return lax.broadcasted_iota(jnp.int32, shape, axis) < sp[slot, 1 + block]


def key_bias(sp, slot, axis):
    shape = (ROWS, 1) if axis == 0 else (1, ROWS)
    parts = [
        jnp.where(live_limit(sp, slot, block, shape, axis), 0.0, NEGATIVE) for block in range(4)
    ]
    return jnp.concatenate(parts, axis=axis)


def fwd_kernel(slot, sp, q0, k0, v0, q1, k1, v1, k2, v2, k3, v3, att, lse):
    bias = key_bias(sp, slot, 1)
    work = []
    for head in range(TOGETHER):
        cols = slice(head * HD, (head + 1) * HD)
        keys = jnp.concatenate([k[0, :, cols] for k in (k0, k1, k2, k3)], axis=0)
        values = jnp.concatenate([v[0, :, cols] for v in (v0, v1, v2, v3)], axis=0)
        for block, q in enumerate((q0, q1)):
            work.append((head, cols, block, mm(q[0, :, cols], keys, NT), values))
    for head, cols, block, products, values in work:
        scores = products * (SCALE * LOG2E) + bias
        peak = jnp.max(scores, axis=1, keepdims=True)
        powers = jnp.exp2(scores - peak)
        total = jnp.sum(powers, axis=1, keepdims=True)
        live = live_limit(sp, slot, block, (ROWS, 1), 0)
        inverse = jnp.where(live, 1.0 / total, 0.0)
        mixed = mm(powers.astype(jnp.bfloat16), values, NN) * inverse
        att[block, :, cols] = mixed.astype(jnp.bfloat16)
        level = jnp.where(live, peak + jnp.log2(total), -NEGATIVE)
        lse[head, :, block * ROWS : (block + 1) * ROWS] = jnp.broadcast_to(level, (ROWS, HD)).T[:8]


def bwd_kernel(
    slot, sp, q0, k0, v0, q1, k1, v1, k2, v2, k3, v3, att, lse, do0, do1, own, r1, r2, r3
):
    keys = jnp.concatenate([k0[0], k1[0], k2[0], k3[0]], axis=0)
    values = jnp.concatenate([v0[0], v1[0], v2[0], v3[0]], axis=0)
    bias = key_bias(sp, slot, 0)
    grad_k = None
    grad_v = None
    for block, (q, do) in enumerate(((q0, do0), (q1, do1))):
        d_rows = do[0]
        scores = mm(keys, q[0], NT) * (SCALE * LOG2E) + bias
        level = lse[0, 0:1, block * ROWS : (block + 1) * ROWS]
        probs = jnp.exp2(scores - level)
        product = d_rows.astype(jnp.float32) * att[block].astype(jnp.float32)
        dots = jnp.sum(product.T, axis=0, keepdims=True)
        d_probs = mm(values, d_rows, NT)
        d_scores = (probs * (d_probs - dots)).astype(jnp.bfloat16)
        v_part = mm(probs.astype(jnp.bfloat16), d_rows, NN)
        k_part = mm(d_scores, q[0], NN)
        grad_k = k_part if block == 0 else grad_k + k_part
        grad_v = v_part if block == 0 else grad_v + v_part
        grad_q = (mm(keys, d_scores, TN) * SCALE).T
        if block == 0:
            own[0] = grad_q
        else:
            r1[0] = grad_q.astype(jnp.bfloat16)
    grad_k = grad_k * SCALE
    own[1] = grad_k[:ROWS]
    own[2] = grad_v[:ROWS]
    r1[1] = grad_k[ROWS : 2 * ROWS].astype(jnp.bfloat16)
    r1[2] = grad_v[ROWS : 2 * ROWS].astype(jnp.bfloat16)
    r2[0] = grad_k[2 * ROWS : 3 * ROWS].astype(jnp.bfloat16)
    r2[1] = grad_v[2 * ROWS : 3 * ROWS].astype(jnp.bfloat16)
    r3[0] = grad_k[3 * ROWS :].astype(jnp.bfloat16)
    r3[1] = grad_v[3 * ROWS :].astype(jnp.bfloat16)


def head_block(lead, index=0, heads=1):
    return pl.BlockSpec((lead, ROWS, heads * HD), lambda h, sp: (index, 0, h))


def section_specs(slot, heads=1):
    def own(member):
        return pl.BlockSpec(
            (1, ROWS, heads * HD),
            lambda h, sp: (slot, 0, (12 * member + HEADS_HALF * sp[0, 0]) // heads + h),
        )

    return [own(0), own(1), own(2)] + [head_block(1, m, heads) for m in (0, 1, 2, 0, 1, 0, 1)]


def sections(qkv, x1, x2, x3):
    return (qkv, qkv, qkv, x1, x1, x1, x2, x2, x3, x3)


LSE_SPEC = pl.BlockSpec((1, 8, 2 * ROWS), lambda h, sp: (h, 0, 0))
PAIRS = HEADS_HALF * 512 * 1024


def attend(sp, slot, qkv, received):
    return pl.pallas_call(
        functools.partial(fwd_kernel, slot),
        grid_spec=pltpu.PrefetchScalarGridSpec(
            num_scalar_prefetch=1,
            grid=(HEADS_HALF // TOGETHER,),
            in_specs=section_specs(slot, TOGETHER),
            out_specs=[
                head_block(2, 0, TOGETHER),
                pl.BlockSpec((TOGETHER, 8, 2 * ROWS), lambda h, sp: (h, 0, 0)),
            ],
        ),
        out_shape=[
            jax.ShapeDtypeStruct((2, ROWS, HALF), jnp.bfloat16),
            jax.ShapeDtypeStruct((HEADS_HALF, 8, 2 * ROWS), jnp.float32),
        ],
        cost_estimate=cost(4 * PAIRS * HD, 5e6, PAIRS),
    )(sp, *sections(qkv, *received))


def attend_back(sp, slot, qkv, received, att, lse, d_own, d_peer):
    d_own_spec = pl.BlockSpec((1, ROWS, HD), lambda h, sp: (0, 0, HEADS_HALF * sp[0, 0] + h))

    def shape(count, kind):
        return jax.ShapeDtypeStruct((count, ROWS, HALF), kind)

    return pl.pallas_call(
        functools.partial(bwd_kernel, slot),
        grid_spec=pltpu.PrefetchScalarGridSpec(
            num_scalar_prefetch=1,
            grid=(HEADS_HALF,),
            in_specs=section_specs(slot) + [head_block(2), LSE_SPEC, d_own_spec, head_block(1)],
            out_specs=[head_block(3), head_block(3), head_block(2), head_block(2)],
        ),
        out_shape=[
            shape(3, jnp.float32),
            shape(3, jnp.bfloat16),
            shape(2, jnp.bfloat16),
            shape(2, jnp.bfloat16),
        ],
        cost_estimate=cost(10 * PAIRS * HD, 1e7, PAIRS),
    )(sp, *sections(qkv, *received), att, lse, d_own, d_peer)


def join_kernel(sp, own, p1, p2, p3, *rest):
    out = rest[-1]
    core = sp[0, 0]
    member = pl.program_id(0)
    crossing = jnp.where(member > 0, 1.0, 0.0)
    mine = own[0] + crossing * p2[0].astype(jnp.float32)
    other = p1[0].astype(jnp.float32) + crossing * p3[0].astype(jnp.float32)
    first = core == 0
    out[0, :, :HALF] = jnp.where(first, mine, other).astype(jnp.bfloat16)
    out[0, :, HALF:] = jnp.where(first, other, mine).astype(jnp.bfloat16)


def join(sp, slot, own, p1, p2, p3, base):
    def piece(shift):
        return pl.BlockSpec((1, ROWS, HALF), lambda m, sp: (jnp.maximum(m - shift, 0), 0, 0))

    in_specs = [piece(0), piece(0), piece(1), piece(1)]
    args = [own, p1, p2, p3]
    aliases = {}
    if base is not None:
        in_specs.append(pl.BlockSpec(memory_space=pl.ANY))
        args.append(base)
        aliases = {5: 0}
    return pl.pallas_call(
        join_kernel,
        grid_spec=pltpu.PrefetchScalarGridSpec(
            num_scalar_prefetch=1,
            grid=(3,),
            in_specs=in_specs,
            out_specs=pl.BlockSpec((1, ROWS, WIDTH), lambda m, sp: (slot, 0, m)),
        ),
        out_shape=jax.ShapeDtypeStruct((2, ROWS, 3 * WIDTH), jnp.bfloat16),
        input_output_aliases=aliases,
        cost_estimate=cost(1e6, 1e7),
    )(sp, *args)


def pick_kernel(order, rows, out):
    def step(slot, carry):
        out[slot] = rows[order[slot]]
        return carry

    lax.fori_loop(0, rows.shape[0], step, 0)


def pick(rows, order):
    whole = pl.BlockSpec(rows.shape, lambda i, order: (0, 0, 0))
    return pl.pallas_call(
        pick_kernel,
        grid_spec=pltpu.PrefetchScalarGridSpec(
            num_scalar_prefetch=1, grid=(1,), in_specs=[whole], out_specs=whole
        ),
        out_shape=jax.ShapeDtypeStruct(rows.shape, rows.dtype),
        cost_estimate=cost(1e6, 2 * rows.size * 2),
        name="pick",
    )(order, rows)


def rows_kernel(sp, cotangent, gate, weight, send, keep, away, near, near_send, total):
    step = pl.program_id(0)
    parts = [
        (cotangent[slot].astype(jnp.float32) * gate[slot : slot + 1]).astype(jnp.bfloat16)
        for slot in range(2)
    ]

    @pl.when(step < 3)
    def _():
        send[0] = parts[0]
        send[1] = parts[1]

    @pl.when(step >= 3)
    def _():
        keep[0] = parts[0]
        keep[1] = parts[1]

    product = mm(jnp.concatenate(parts, axis=0), weight[...], NT)

    @pl.when(step == 0)
    def _():
        total[...] = product

    @pl.when((step > 0) & (step < 5))
    def _():
        total[...] += product

    @pl.when(step == 5)
    def _():
        rows = (total[...] + product).astype(jnp.bfloat16)
        near[...] = rows[:ROWS]
        away[...] = rows[ROWS:]
        near_send[0] = jnp.where(sp[0, 0] == 0, rows[:ROWS, HALF:], rows[:ROWS, :HALF])


def scaled_rows(sp, cotangent, gate, out_weight):
    cols = D // 6

    def place(step, sp):
        core = sp[0, 0]
        return jnp.where(step < 3, 3 * (1 - core), 3 * core - 3) + step

    def whole(*shape):
        return pl.BlockSpec(shape, lambda k, sp: (0,) * len(shape))

    def shape(*dims):
        return jax.ShapeDtypeStruct(dims, jnp.bfloat16)

    return pl.pallas_call(
        rows_kernel,
        grid_spec=pltpu.PrefetchScalarGridSpec(
            num_scalar_prefetch=1,
            grid=(6,),
            in_specs=[
                pl.BlockSpec((2, ROWS, cols), lambda k, sp: (0, 0, place(k, sp))),
                pl.BlockSpec((2, cols), lambda k, sp: (0, place(k, sp))),
                pl.BlockSpec((WIDTH, cols), lambda k, sp: (0, place(k, sp))),
            ],
            out_specs=[
                pl.BlockSpec((2, ROWS, cols), lambda k, sp: (0, 0, jnp.minimum(k, 2))),
                pl.BlockSpec((2, ROWS, cols), lambda k, sp: (0, 0, jnp.maximum(k - 3, 0))),
                whole(ROWS, WIDTH),
                whole(ROWS, WIDTH),
                whole(1, ROWS, HALF),
            ],
            scratch_shapes=[pltpu.VMEM((2 * ROWS, WIDTH), jnp.float32)],
        ),
        out_shape=[
            shape(2, ROWS, D // 2),
            shape(2, ROWS, D // 2),
            shape(ROWS, WIDTH),
            shape(ROWS, WIDTH),
            shape(1, ROWS, HALF),
        ],
        cost_estimate=cost(2 * 512 * WIDTH * D, 1.7e7),
        name="scaled_rows",
    )(sp, cotangent, gate, out_weight)


def project_kernel(sp, a0, a1, b0, b1, w_mine, w_other, gate, cotangent, mixed, gate_grad):
    mine = jnp.concatenate([a0[0], a1[0]], axis=0)
    other = jnp.concatenate([b0[0], b1[0]], axis=0)
    outputs = mm(mine, w_mine[...], NN) + mm(other, w_other[...], NN)
    for slot in range(2):
        rows = outputs[slot * ROWS : (slot + 1) * ROWS]
        mixed[slot] = (rows * gate[slot : slot + 1]).astype(jnp.bfloat16)
        gate_grad[slot : slot + 1] = jnp.sum(
            cotangent[slot].astype(jnp.float32) * rows, axis=0, keepdims=True
        )


def project(sp, mine, other, out_weight, gate, cotangent):
    cols = 512

    def rows(index):
        return pl.BlockSpec((1, ROWS, HALF), lambda d, sp: (index, 0, 0))

    wide = pl.BlockSpec((2, ROWS, cols), lambda d, sp: (0, 0, d))
    thin = pl.BlockSpec((2, cols), lambda d, sp: (0, d))
    return pl.pallas_call(
        project_kernel,
        grid_spec=pltpu.PrefetchScalarGridSpec(
            num_scalar_prefetch=1,
            grid=(D // cols,),
            in_specs=[
                rows(0),
                rows(0),
                rows(1),
                rows(1),
                pl.BlockSpec((HALF, cols), lambda d, sp: (sp[0, 0], d)),
                pl.BlockSpec((HALF, cols), lambda d, sp: (1 - sp[0, 0], d)),
                thin,
                wide,
            ],
            out_specs=[wide, thin],
        ),
        out_shape=[
            jax.ShapeDtypeStruct((2, ROWS, D), jnp.bfloat16),
            jax.ShapeDtypeStruct((2, D), jnp.float32),
        ],
        cost_estimate=cost(2 * 512 * WIDTH * D, 1.6e7),
        name="project",
    )(sp, mine[0], mine[1], other[0], other[1], out_weight, out_weight, gate, cotangent)


def weigh_kernel(sp, scaled_own, scaled_peer, a0, a1, b0, b1, *rest):
    outs, product = rest[:8], rest[8]
    step = pl.program_id(0)
    left = jnp.concatenate(
        [scaled_own[0], scaled_peer[0], scaled_own[1], scaled_peer[1]], axis=0
    )
    mine = jnp.concatenate([a0[0], a0[1], a1[0], a1[1]], axis=0)
    other = jnp.concatenate([b0[1], b0[0], b1[1], b1[0]], axis=0)
    first = sp[0, 0] == 0
    by_x = mm(left, jnp.where(first, mine, other), TN).astype(jnp.bfloat16)
    for x_step in range(4):

        @pl.when(step == x_step)
        def _():
            outs[x_step][...] = by_x

    product[...] = mm(left, jnp.where(first, other, mine), TN)
    for y_step in range(4):
        start = pl.multiple_of((sp[1, 5] ^ y_step) * SHARE, 8)
        rows = product[pl.ds(start, SHARE), :].astype(jnp.bfloat16)
        outs[4 + y_step][sp[0, 5] ^ step] = rows


def weigh(sp, scaled, scaled_peer, mine, other):
    rows = D // 8
    pair = pl.BlockSpec((2, ROWS, HALF), lambda d, sp: (0, 0, 0))
    wide = pl.BlockSpec((2, ROWS, rows), lambda d, sp: (0, 0, sp[0, 5] ^ d))
    return pl.pallas_call(
        weigh_kernel,
        grid_spec=pltpu.PrefetchScalarGridSpec(
            num_scalar_prefetch=1,
            grid=(4,),
            in_specs=[wide, wide, pair, pair, pair, pair],
            out_specs=[pl.BlockSpec((rows, HALF), lambda d, sp: (0, 0))] * 4
            + [pl.BlockSpec((4, SHARE, HALF), lambda d, sp: (0, 0, 0))] * 4,
            scratch_shapes=[pltpu.VMEM((rows, HALF), jnp.float32)],
        ),
        out_shape=[jax.ShapeDtypeStruct((rows, HALF), jnp.bfloat16)] * 4
        + [jax.ShapeDtypeStruct((4, SHARE, HALF), jnp.bfloat16)] * 4,
        cost_estimate=cost(2 * 1024 * WIDTH * D // 2, 1.2e7),
        name="weigh",
    )(sp, scaled, scaled_peer, mine[0], mine[1], other[0], other[1])


def along_x(x, step):
    return lax.ppermute(x, "dp", [(g, g ^ (step << 3)) for g in range(32)])


def along_y(x, step):
    return lax.ppermute(x, "dp", [(g, g ^ (step << 1)) for g in range(32)])


def add_up(refs):
    total = refs[0][...].astype(jnp.float32)
    for ref in refs[1:]:
        total = total + ref[...].astype(jnp.float32)
    return total


def part_kernel(sp, *refs):
    by_x, by_y, outs, total = refs[:4], refs[4:8], refs[8:16], refs[16]
    total[...] = add_up(by_x)
    for step in range(4):
        start = pl.multiple_of((sp[1, 5] ^ step) * SHARE, 8)
        outs[step][...] = total[pl.ds(start, SHARE), :].astype(jnp.bfloat16)
    for step in range(4):
        place = sp[0, 5] ^ step
        rows = by_y[0][place].astype(jnp.float32)
        for ref in by_y[1:]:
            rows = rows + ref[place].astype(jnp.float32)
        outs[4 + step][...] = rows.astype(jnp.bfloat16)


def sum_parts(sp, by_x, by_y):
    cols = HALF // 2
    share = pl.BlockSpec((SHARE, cols), lambda i, sp: (0, i))
    return pl.pallas_call(
        part_kernel,
        grid_spec=pltpu.PrefetchScalarGridSpec(
            num_scalar_prefetch=1,
            grid=(2,),
            in_specs=[pl.BlockSpec((4 * SHARE, cols), lambda i, sp: (0, i))] * 4
            + [pl.BlockSpec((4, SHARE, cols), lambda i, sp: (0, 0, i))] * 4,
            out_specs=[share] * 8,
            scratch_shapes=[pltpu.VMEM((4 * SHARE, cols), jnp.float32)],
        ),
        out_shape=[jax.ShapeDtypeStruct((SHARE, HALF), jnp.bfloat16)] * 8,
        cost_estimate=cost(5e6, 6e6),
        name="sum_parts",
    )(sp, *by_x, *by_y)


def final_moves(step):
    moves = []
    for xy in range(16):
        for z_low in range(2):
            for z_high in range(2):
                for core in range(2):
                    source = 4 * (2 * xy + z_low) + 2 * z_high + core
                    target = 4 * (16 * core + xy) + ((2 * z_low + z_high) ^ step)
                    moves.append((source, target))
    return moves


def sum_kernel(sp, *refs):
    low, high, outs, total = refs[:4], refs[4:8], refs[8:12], refs[12]
    total[:, :HALF] = add_up(low)
    total[:, HALF:] = add_up(high)
    count = SHARE // 4
    for step, out in enumerate(outs):
        start = pl.multiple_of((sp[1, 0] ^ step) * count, 8)
        out[...] = total[pl.ds(start, count), :].astype(jnp.bfloat16)


def sum_weights(sp, low, high):
    def whole(rows, cols):
        return pl.BlockSpec((rows, cols), lambda i, sp: (0, 0))

    return pl.pallas_call(
        sum_kernel,
        grid_spec=pltpu.PrefetchScalarGridSpec(
            num_scalar_prefetch=1,
            grid=(1,),
            in_specs=[whole(SHARE, HALF)] * 8,
            out_specs=[whole(SHARE // 4, WIDTH)] * 4,
            scratch_shapes=[pltpu.VMEM((SHARE, WIDTH), jnp.float32)],
        ),
        out_shape=[jax.ShapeDtypeStruct((SHARE // 4, WIDTH), jnp.bfloat16)] * 4,
        cost_estimate=cost(1e6, 2e6),
        name="sum_weights",
    )(sp, *low, *high)


def finish_weights(quarters):
    pieces = [
        lax.ppermute(quarter, ("dp", "seq"), final_moves(step)).astype(jnp.float32)
        for step, quarter in enumerate(quarters)
    ]
    return (pieces[0] + pieces[1] + pieces[2] + pieces[3]).T


def after(value, *others):
    return lax.optimization_barrier((value, *others))[0]


def spread_out(rows):
    groups = lax.axis_size("dp")
    portions = rows.reshape(groups, -1, rows.shape[-1])
    return lax.all_to_all(portions, "dp", split_axis=0, concat_axis=0, tiled=True)


def land(arranged, shape):
    landed = lax.all_to_all(arranged, "dp", split_axis=0, concat_axis=0, tiled=True)
    return landed.reshape(shape)


def body(qkv, gate, cotangent, out_weight, clip_lengths, text_lengths, plan):
    groups = lax.axis_size("dp")
    group_index = lax.axis_index("dp")
    seq_index = lax.axis_index("seq")
    core = seq_index & 1
    z_place = 2 * (group_index & 1) + (seq_index >> 1)
    ordinal = jnp.arange(groups, dtype=jnp.int32)
    inverse = jnp.sum(jnp.where(plan[None, :] == ordinal[:, None], ordinal[None, :], 0), axis=1)

    quarters = seq_index ^ jnp.arange(4, dtype=jnp.int32)
    text = lax.dynamic_slice_in_dim(text_lengths, 2 * group_index, 2)[:, None]
    video = lax.dynamic_slice_in_dim(clip_lengths, 2 * group_index, 2)[:, None]
    limits = jnp.where(quarters[None] == 0, text, video - (quarters[None] - 1) * ROWS)
    place = jnp.stack([core, z_place]).astype(jnp.int32)[:, None]
    plane = jnp.stack([group_index >> 3, (group_index >> 1) & 3]).astype(jnp.int32)[:, None]
    sp = jnp.concatenate([place, limits.astype(jnp.int32), plane], axis=1)
    first = core == 0

    def to_core(rows):
        other = jnp.where(first, rows[:, HALF:], rows[:, :HALF])
        return swap(other[None], 1)

    received = [None, None]
    d_own, d_peer = [None, None], [None, None]
    att, lse = [None, None], [None, None]

    s1, s2, s3 = prep(sp, qkv, 1)
    received[1] = (swap(s1, 1), swap(s2, 2), swap(s3, 3))
    scaled_send, scaled, away, near, near_send = scaled_rows(
        after(sp, s2), cotangent, gate, out_weight
    )
    d_spread = spread_out(away)
    s1, s2, s3 = prep(after(sp, away), qkv, 0)
    near_keys = (swap(s1, 1), swap(s3, 3))
    received[0] = (near_keys[0], swap(s2, 2), near_keys[1])
    d_own[0], d_peer[0] = near[None], swap(near_send, 1)
    scaled_peer = swap(scaled_send, 1)

    d_picked = pick(d_spread, after(plan, s2))
    landed = land(d_picked, (ROWS, WIDTH))
    att[1], lse[1] = attend(after(sp, d_picked), 1, qkv, received[1])
    d_own[1], d_peer[1] = landed[None], to_core(landed)
    att_spread = spread_out(after(att[1], landed).reshape(2 * ROWS, HALF))

    def back(sp, slot):
        return attend_back(
            sp, slot, qkv, received[slot], att[slot], lse[slot], d_own[slot], d_peer[slot]
        )

    own_1, r1, r2, r3 = back(sp, 1)
    pieces_1 = (swap(r1, 1), swap(r3, 3))
    pieces_1 = (pieces_1[0], swap(r2, 2), pieces_1[1])
    att[0], lse[0] = attend(after(sp, r2), 0, qkv, received[0])
    att_other = [swap(att[0], 1)]
    picked = pick(att_spread, after(inverse, lse[0]))
    moved = land(picked, (2, ROWS, HALF))
    own_0, *sent_0 = back(after(sp, picked), 0)
    pieces_0 = [swap(rows, 1 + i) for i, rows in enumerate(sent_0)]
    balanced = [att[0], moved]
    att_other.append(swap(moved, 1))
    *partial, = weigh(after(sp, sent_0[1]), scaled, scaled_peer, balanced, att_other)
    by_x, by_y = partial[:4], partial[4:]
    for step in (2, 1, 3):
        by_x[step] = along_x(by_x[step], step)
        by_y[step] = along_y(by_y[step], step)
    mixed, gate_part = project(
        after(sp, partial[0]), balanced, att_other, out_weight, gate, cotangent
    )
    gate_grad = gate_part + swap(gate_part, 1) + swap(gate_part, 2) + swap(gate_part, 3)
    grads = join(after(sp, gate_part), 1, own_1, *pieces_1, None)
    parts = list(sum_parts(after(sp, grads), by_x, by_y))
    low = parts[:1] + [along_y(parts[step], step) for step in (1, 2, 3)]
    high = parts[4:5] + [along_x(parts[4 + step], step) for step in (1, 2, 3)]
    quarters = sum_weights(sp, low, high)
    weight_grad = finish_weights(quarters)
    grads = join(after(sp, quarters[0]), 0, own_0, *pieces_0, grads)
    return (mixed, gate_grad, weight_grad, grads)


def solution(mesh):
    in_specs = (P("dp", "seq", None), P("dp", None), P("dp", "seq", None), P(), P(), P(), P())
    out_specs = (P("dp", "seq", None), P("dp", None), P(None, ("dp", "seq")), P("dp", "seq", None))
    return jax.shard_map(body, mesh=mesh, in_specs=in_specs, out_specs=out_specs, check_vma=False)
```

```python
import functools

import jax
import jax.numpy as jnp
from jax import lax
from jax.experimental import pallas as pl
from jax.experimental.pallas import tpu as pltpu
from jax.sharding import PartitionSpec as P


HD = 128
ROWS = 256
HEADS_HALF = 6
HALF = HEADS_HALF * HD
WIDTH = 2 * HALF
TOGETHER = 2
TOGETHER_BACK = 2
SHARE = 96
D = 3072
NEGATIVE = -1e30
LOG2E = 1.4426950408889634
SCALE = HD**-0.5

NT = (((1,), (1,)), ((), ()))
NN = (((1,), (0,)), ((), ()))
TN = (((0,), (0,)), ((), ()))


def mm(a, b, dims):
    return lax.dot_general(a, b, dims, preferred_element_type=jnp.float32)


def cost(flops, nbytes, transcendentals=0):
    return pl.CostEstimate(
        flops=int(flops), bytes_accessed=int(nbytes), transcendentals=int(transcendentals)
    )


def swap(x, step):
    return lax.ppermute(x, "seq", [(i, i ^ step) for i in range(4)])


def prep_kernel(sp, qo, ko, vo, kc, vc, s1, s2, s3):
    s1[0] = qo[0]
    s1[1] = ko[0]
    s1[2] = vo[0]
    s2[0] = kc[0]
    s2[1] = vc[0]
    s3[0] = ko[0]
    s3[1] = vo[0]


def prep(sp, qkv, slot):
    rows = ROWS // 2

    def half(member, other):
        def index(r, sp):
            core = sp[0, 0]
            return (slot, r, 2 * member + (1 - core if other else core))

        return pl.BlockSpec((1, rows, HALF), index)

    def out(count):
        return pl.BlockSpec((count, rows, HALF), lambda r, sp: (0, r, 0))

    def shape(count):
        return jax.ShapeDtypeStruct((count, ROWS, HALF), jnp.bfloat16)

    return pl.pallas_call(
        prep_kernel,
        grid_spec=pltpu.PrefetchScalarGridSpec(
            num_scalar_prefetch=1,
            grid=(2,),
            in_specs=[half(0, True), half(1, True), half(2, True), half(1, False), half(2, False)],
            out_specs=[out(3), out(2), out(2)],
        ),
        out_shape=[shape(3), shape(2), shape(2)],
        cost_estimate=cost(1e6, 5e6),
    )(sp, qkv, qkv, qkv, qkv, qkv)


def live_limit(sp, slot, block, shape, axis):
    return lax.broadcasted_iota(jnp.int32, shape, axis) < sp[slot, 1 + block]


def key_bias(sp, slot, axis):
    shape = (ROWS, 1) if axis == 0 else (1, ROWS)
    parts = [
        jnp.where(live_limit(sp, slot, block, shape, axis), 0.0, NEGATIVE) for block in range(4)
    ]
    return jnp.concatenate(parts, axis=axis)


def fwd_kernel(slot, sp, q0, k0, v0, q1, k1, v1, k2, v2, k3, v3, att, lse):
    bias = key_bias(sp, slot, 1)
    work = []
    for head in range(TOGETHER):
        cols = slice(head * HD, (head + 1) * HD)
        keys = jnp.concatenate([k[0, :, cols] for k in (k0, k1, k2, k3)], axis=0)
        values = jnp.concatenate([v[0, :, cols] for v in (v0, v1, v2, v3)], axis=0)
        for block, q in enumerate((q0, q1)):
            work.append((head, cols, block, mm(q[0, :, cols], keys, NT), values))
    for head, cols, block, products, values in work:
        scores = products * (SCALE * LOG2E) + bias
        peak = jnp.max(scores, axis=1, keepdims=True)
        powers = jnp.exp2(scores - peak)
        total = jnp.sum(powers, axis=1, keepdims=True)
        live = live_limit(sp, slot, block, (ROWS, 1), 0)
        inverse = jnp.where(live, 1.0 / total, 0.0)
        mixed = mm(powers.astype(jnp.bfloat16), values, NN) * inverse
        att[block, :, cols] = mixed.astype(jnp.bfloat16)
        level = jnp.where(live, peak + jnp.log2(total), -NEGATIVE)
        lse[head, :, block * ROWS : (block + 1) * ROWS] = jnp.broadcast_to(level, (ROWS, HD)).T[:8]


def bwd_kernel(
    slot, sp, q0, k0, v0, q1, k1, v1, k2, v2, k3, v3, att, lse, do0, do1, own, r1, r2, r3
):
    bias = key_bias(sp, slot, 0)
    low = jnp.bfloat16
    for head in range(TOGETHER_BACK):
        cols = slice(head * HD, (head + 1) * HD)
        keys = jnp.concatenate([k[0, :, cols] for k in (k0, k1, k2, k3)], axis=0)
        values = jnp.concatenate([v[0, :, cols] for v in (v0, v1, v2, v3)], axis=0)
        grad_k = None
        grad_v = None
        for block, (q, do) in enumerate(((q0, do0), (q1, do1))):
            q_rows = q[0, :, cols]
            d_rows = do[0, :, cols]
            scores = mm(keys, q_rows, NT) * (SCALE * LOG2E) + bias
            level = lse[head, 0:1, block * ROWS : (block + 1) * ROWS]
            probs = jnp.exp2(scores - level)
            product = d_rows.astype(jnp.float32) * att[block, :, cols].astype(jnp.float32)
            dots = jnp.sum(product.T, axis=0, keepdims=True)
            d_probs = mm(values, d_rows, NT)
            d_scores = (probs * (d_probs - dots)).astype(low)
            v_part = mm(probs.astype(low), d_rows, NN)
            k_part = mm(d_scores, q_rows, NN)
            grad_k = k_part if block == 0 else grad_k + k_part
            grad_v = v_part if block == 0 else grad_v + v_part
            grad_q = (mm(keys, d_scores, TN) * SCALE).T
            if block == 0:
                own[0, :, cols] = grad_q
            else:
                r1[0, :, cols] = grad_q.astype(low)
        grad_k = grad_k * SCALE
        own[1, :, cols] = grad_k[:ROWS]
        own[2, :, cols] = grad_v[:ROWS]
        r1[1, :, cols] = grad_k[ROWS : 2 * ROWS].astype(low)
        r1[2, :, cols] = grad_v[ROWS : 2 * ROWS].astype(low)
        r2[0, :, cols] = grad_k[2 * ROWS : 3 * ROWS].astype(low)
        r2[1, :, cols] = grad_v[2 * ROWS : 3 * ROWS].astype(low)
        r3[0, :, cols] = grad_k[3 * ROWS :].astype(low)
        r3[1, :, cols] = grad_v[3 * ROWS :].astype(low)


def head_block(lead, index=0, heads=1):
    return pl.BlockSpec((lead, ROWS, heads * HD), lambda h, sp: (index, 0, h))


def section_specs(slot, heads=1):
    def own(member):
        return pl.BlockSpec(
            (1, ROWS, heads * HD),
            lambda h, sp: (slot, 0, (12 * member + HEADS_HALF * sp[0, 0]) // heads + h),
        )

    return [own(0), own(1), own(2)] + [head_block(1, m, heads) for m in (0, 1, 2, 0, 1, 0, 1)]


def sections(qkv, x1, x2, x3):
    return (qkv, qkv, qkv, x1, x1, x1, x2, x2, x3, x3)


PAIRS = HEADS_HALF * 512 * 1024


def attend(sp, slot, qkv, received):
    return pl.pallas_call(
        functools.partial(fwd_kernel, slot),
        grid_spec=pltpu.PrefetchScalarGridSpec(
            num_scalar_prefetch=1,
            grid=(HEADS_HALF // TOGETHER,),
            in_specs=section_specs(slot, TOGETHER),
            out_specs=[
                head_block(2, 0, TOGETHER),
                pl.BlockSpec((TOGETHER, 8, 2 * ROWS), lambda h, sp: (h, 0, 0)),
            ],
        ),
        out_shape=[
            jax.ShapeDtypeStruct((2, ROWS, HALF), jnp.bfloat16),
            jax.ShapeDtypeStruct((HEADS_HALF, 8, 2 * ROWS), jnp.float32),
        ],
        cost_estimate=cost(4 * PAIRS * HD, 5e6, PAIRS),
    )(sp, *sections(qkv, *received))


def attend_back(sp, slot, qkv, received, att, lse, d_own, d_peer):
    heads = TOGETHER_BACK
    d_own_spec = pl.BlockSpec(
        (1, ROWS, heads * HD), lambda h, sp: (0, 0, HEADS_HALF // heads * sp[0, 0] + h)
    )

    def shape(count, kind):
        return jax.ShapeDtypeStruct((count, ROWS, HALF), kind)

    def piece(count):
        return head_block(count, 0, heads)

    return pl.pallas_call(
        functools.partial(bwd_kernel, slot),
        grid_spec=pltpu.PrefetchScalarGridSpec(
            num_scalar_prefetch=1,
            grid=(HEADS_HALF // heads,),
            in_specs=section_specs(slot, heads)
            + [
                piece(2),
                pl.BlockSpec((heads, 8, 2 * ROWS), lambda h, sp: (h, 0, 0)),
                d_own_spec,
                piece(1),
            ],
            out_specs=[piece(3), piece(3), piece(2), piece(2)],
        ),
        out_shape=[
            shape(3, jnp.float32),
            shape(3, jnp.bfloat16),
            shape(2, jnp.bfloat16),
            shape(2, jnp.bfloat16),
        ],
        cost_estimate=cost(10 * PAIRS * HD, 1e7, PAIRS),
    )(sp, *sections(qkv, *received), att, lse, d_own, d_peer)


def join_kernel(sp, own, p1, p2, p3, *rest):
    out = rest[-1]
    core = sp[0, 0]
    member = pl.program_id(0)
    crossing = jnp.where(member > 0, 1.0, 0.0)
    mine = own[0] + crossing * p2[0].astype(jnp.float32)
    other = p1[0].astype(jnp.float32) + crossing * p3[0].astype(jnp.float32)
    first = core == 0
    out[0, :, :HALF] = jnp.where(first, mine, other).astype(jnp.bfloat16)
    out[0, :, HALF:] = jnp.where(first, other, mine).astype(jnp.bfloat16)


def join(sp, slot, own, p1, p2, p3, base):
    def piece(shift):
        return pl.BlockSpec((1, ROWS, HALF), lambda m, sp: (jnp.maximum(m - shift, 0), 0, 0))

    in_specs = [piece(0), piece(0), piece(1), piece(1)]
    args = [own, p1, p2, p3]
    aliases = {}
    if base is not None:
        in_specs.append(pl.BlockSpec(memory_space=pl.ANY))
        args.append(base)
        aliases = {5: 0}
    return pl.pallas_call(
        join_kernel,
        grid_spec=pltpu.PrefetchScalarGridSpec(
            num_scalar_prefetch=1,
            grid=(3,),
            in_specs=in_specs,
            out_specs=pl.BlockSpec((1, ROWS, WIDTH), lambda m, sp: (slot, 0, m)),
        ),
        out_shape=jax.ShapeDtypeStruct((2, ROWS, 3 * WIDTH), jnp.bfloat16),
        input_output_aliases=aliases,
        cost_estimate=cost(1e6, 1e7),
    )(sp, *args)


def pick_kernel(order, rows, out):
    def step(slot, carry):
        out[slot] = rows[order[slot]]
        return carry

    lax.fori_loop(0, rows.shape[0], step, 0)


def pick(rows, order):
    whole = pl.BlockSpec(rows.shape, lambda i, order: (0, 0, 0))
    return pl.pallas_call(
        pick_kernel,
        grid_spec=pltpu.PrefetchScalarGridSpec(
            num_scalar_prefetch=1, grid=(1,), in_specs=[whole], out_specs=whole
        ),
        out_shape=jax.ShapeDtypeStruct(rows.shape, rows.dtype),
        cost_estimate=cost(1e6, 2 * rows.size * 2),
        name="pick",
    )(order, rows)


def rows_kernel(slot, sp, cotangent, gate, weight, send, keep, rows, total):
    step = pl.program_id(0)
    scaled = (cotangent[0].astype(jnp.float32) * gate[slot : slot + 1]).astype(jnp.bfloat16)

    @pl.when(step < 2)
    def _():
        send[...] = scaled

    @pl.when(step >= 2)
    def _():
        keep[...] = scaled

    product = mm(scaled, weight[...], NT)

    @pl.when(step == 0)
    def _():
        total[...] = product

    @pl.when((step > 0) & (step < 3))
    def _():
        total[...] += product

    @pl.when(step == 3)
    def _():
        rows[...] = (total[...] + product).astype(jnp.bfloat16)


def scaled_rows(sp, slot, cotangent, gate, out_weight):
    cols = D // 4

    def place(step, sp):
        core = sp[0, 0]
        return jnp.where(step < 2, 2 * (1 - core), 2 * core - 2) + step

    def shape(cols):
        return jax.ShapeDtypeStruct((ROWS, cols), jnp.bfloat16)

    return pl.pallas_call(
        functools.partial(rows_kernel, slot),
        grid_spec=pltpu.PrefetchScalarGridSpec(
            num_scalar_prefetch=1,
            grid=(4,),
            in_specs=[
                pl.BlockSpec((1, ROWS, cols), lambda k, sp: (slot, 0, place(k, sp))),
                pl.BlockSpec((2, cols), lambda k, sp: (0, place(k, sp))),
                pl.BlockSpec((WIDTH, cols), lambda k, sp: (0, place(k, sp))),
            ],
            out_specs=[
                pl.BlockSpec((ROWS, cols), lambda k, sp: (0, jnp.minimum(k, 1))),
                pl.BlockSpec((ROWS, cols), lambda k, sp: (0, jnp.maximum(k - 2, 0))),
                pl.BlockSpec((ROWS, WIDTH), lambda k, sp: (0, 0)),
            ],
            scratch_shapes=[pltpu.VMEM((ROWS, WIDTH), jnp.float32)],
        ),
        out_shape=[shape(D // 2), shape(D // 2), shape(WIDTH)],
        cost_estimate=cost(2 * 256 * WIDTH * D, 1.3e7),
    )(sp, cotangent, gate, out_weight)


def project_kernel(sp, a0, a1, b0, b1, w_mine, w_other, gate, cotangent, mixed, gate_grad):
    mine = jnp.concatenate([a0[0], a1[0]], axis=0)
    other = jnp.concatenate([b0[0], b1[0]], axis=0)
    outputs = mm(mine, w_mine[...], NN) + mm(other, w_other[...], NN)
    for slot in range(2):
        rows = outputs[slot * ROWS : (slot + 1) * ROWS]
        mixed[slot] = (rows * gate[slot : slot + 1]).astype(jnp.bfloat16)
        gate_grad[slot : slot + 1] = jnp.sum(
            cotangent[slot].astype(jnp.float32) * rows, axis=0, keepdims=True
        )


def project(sp, mine, other, out_weight, gate, cotangent):
    cols = 1024

    def rows(index):
        return pl.BlockSpec((1, ROWS, HALF), lambda d, sp: (index, 0, 0))

    wide = pl.BlockSpec((2, ROWS, cols), lambda d, sp: (0, 0, d))
    thin = pl.BlockSpec((2, cols), lambda d, sp: (0, d))
    return pl.pallas_call(
        project_kernel,
        grid_spec=pltpu.PrefetchScalarGridSpec(
            num_scalar_prefetch=1,
            grid=(D // cols,),
            in_specs=[
                rows(0),
                rows(0),
                rows(1),
                rows(1),
                pl.BlockSpec((HALF, cols), lambda d, sp: (sp[0, 0], d)),
                pl.BlockSpec((HALF, cols), lambda d, sp: (1 - sp[0, 0], d)),
                thin,
                wide,
            ],
            out_specs=[wide, thin],
        ),
        out_shape=[
            jax.ShapeDtypeStruct((2, ROWS, D), jnp.bfloat16),
            jax.ShapeDtypeStruct((2, D), jnp.float32),
        ],
        cost_estimate=cost(2 * 512 * WIDTH * D, 1.6e7),
        name="project",
    )(sp, mine[0], mine[1], other[0], other[1], out_weight, out_weight, gate, cotangent)


def weigh_kernel(sp, own0, peer0, own1, peer1, a0, a1, b0, b1, *rest):
    outs, product = rest[:8], rest[8]
    step = pl.program_id(0)
    left = jnp.concatenate([own0[...], peer0[...], own1[...], peer1[...]], axis=0)
    mine = jnp.concatenate([a0[0], a0[1], a1[0], a1[1]], axis=0)
    other = jnp.concatenate([b0[1], b0[0], b1[1], b1[0]], axis=0)
    first = sp[0, 0] == 0
    by_x = mm(left, jnp.where(first, mine, other), TN).astype(jnp.bfloat16)
    for x_step in range(4):

        @pl.when(step == x_step)
        def _():
            outs[x_step][...] = by_x

    product[...] = mm(left, jnp.where(first, other, mine), TN)
    for y_step in range(4):
        start = pl.multiple_of((sp[1, 5] ^ y_step) * SHARE, 8)
        rows = product[pl.ds(start, SHARE), :].astype(jnp.bfloat16)
        outs[4 + y_step][sp[0, 5] ^ step] = rows


def weigh(sp, scaled, mine, other):
    rows = D // 8
    pair = pl.BlockSpec((2, ROWS, HALF), lambda d, sp: (0, 0, 0))
    wide = pl.BlockSpec((ROWS, rows), lambda d, sp: (0, sp[0, 5] ^ d))
    return pl.pallas_call(
        weigh_kernel,
        grid_spec=pltpu.PrefetchScalarGridSpec(
            num_scalar_prefetch=1,
            grid=(4,),
            in_specs=[wide] * 4 + [pair] * 4,
            out_specs=[pl.BlockSpec((rows, HALF), lambda d, sp: (0, 0))] * 4
            + [pl.BlockSpec((4, SHARE, HALF), lambda d, sp: (0, 0, 0))] * 4,
            scratch_shapes=[pltpu.VMEM((rows, HALF), jnp.float32)],
        ),
        out_shape=[jax.ShapeDtypeStruct((rows, HALF), jnp.bfloat16)] * 4
        + [jax.ShapeDtypeStruct((4, SHARE, HALF), jnp.bfloat16)] * 4,
        cost_estimate=cost(2 * 1024 * WIDTH * D // 2, 1.2e7),
        name="weigh",
    )(sp, *scaled, mine[0], mine[1], other[0], other[1])


def along_x(x, step):
    return lax.ppermute(x, "dp", [(g, g ^ (step << 3)) for g in range(32)])


def along_y(x, step):
    return lax.ppermute(x, "dp", [(g, g ^ (step << 1)) for g in range(32)])


def add_up(refs):
    total = refs[0][...].astype(jnp.float32)
    for ref in refs[1:]:
        total = total + ref[...].astype(jnp.float32)
    return total


def part_kernel(sp, *refs):
    by_x, by_y, outs, total = refs[:4], refs[4:8], refs[8:16], refs[16]
    total[...] = add_up(by_x)
    for step in range(4):
        start = pl.multiple_of((sp[1, 5] ^ step) * SHARE, 8)
        outs[step][...] = total[pl.ds(start, SHARE), :].astype(jnp.bfloat16)
    for step in range(4):
        place = sp[0, 5] ^ step
        rows = by_y[0][place].astype(jnp.float32)
        for ref in by_y[1:]:
            rows = rows + ref[place].astype(jnp.float32)
        outs[4 + step][...] = rows.astype(jnp.bfloat16)


def sum_parts(sp, by_x, by_y):
    cols = HALF // 2
    share = pl.BlockSpec((SHARE, cols), lambda i, sp: (0, i))
    return pl.pallas_call(
        part_kernel,
        grid_spec=pltpu.PrefetchScalarGridSpec(
            num_scalar_prefetch=1,
            grid=(2,),
            in_specs=[pl.BlockSpec((4 * SHARE, cols), lambda i, sp: (0, i))] * 4
            + [pl.BlockSpec((4, SHARE, cols), lambda i, sp: (0, 0, i))] * 4,
            out_specs=[share] * 8,
            scratch_shapes=[pltpu.VMEM((4 * SHARE, cols), jnp.float32)],
        ),
        out_shape=[jax.ShapeDtypeStruct((SHARE, HALF), jnp.bfloat16)] * 8,
        cost_estimate=cost(5e6, 6e6),
        name="sum_parts",
    )(sp, *by_x, *by_y)


def final_moves(step):
    moves = []
    for xy in range(16):
        for z_low in range(2):
            for z_high in range(2):
                for core in range(2):
                    source = 4 * (2 * xy + z_low) + 2 * z_high + core
                    target = 4 * (16 * core + xy) + ((2 * z_low + z_high) ^ step)
                    moves.append((source, target))
    return moves


def sum_kernel(sp, *refs):
    low, high, outs, total = refs[:4], refs[4:8], refs[8:12], refs[12]
    total[:, :HALF] = add_up(low)
    total[:, HALF:] = add_up(high)
    count = SHARE // 4
    for step, out in enumerate(outs):
        start = pl.multiple_of((sp[1, 0] ^ step) * count, 8)
        out[...] = total[pl.ds(start, count), :].astype(jnp.bfloat16)


def sum_weights(sp, low, high):
    def whole(rows, cols):
        return pl.BlockSpec((rows, cols), lambda i, sp: (0, 0))

    return pl.pallas_call(
        sum_kernel,
        grid_spec=pltpu.PrefetchScalarGridSpec(
            num_scalar_prefetch=1,
            grid=(1,),
            in_specs=[whole(SHARE, HALF)] * 8,
            out_specs=[whole(SHARE // 4, WIDTH)] * 4,
            scratch_shapes=[pltpu.VMEM((SHARE, WIDTH), jnp.float32)],
        ),
        out_shape=[jax.ShapeDtypeStruct((SHARE // 4, WIDTH), jnp.bfloat16)] * 4,
        cost_estimate=cost(1e6, 2e6),
        name="sum_weights",
    )(sp, *low, *high)


def finish_weights(quarters):
    pieces = [
        lax.ppermute(quarter, ("dp", "seq"), final_moves(step)).astype(jnp.float32)
        for step, quarter in enumerate(quarters)
    ]
    return (pieces[0] + pieces[1] + pieces[2] + pieces[3]).T


def after(value, *others):
    return lax.optimization_barrier((value, *others))[0]


def spread_out(rows):
    groups = lax.axis_size("dp")
    portions = rows.reshape(groups, -1, rows.shape[-1])
    return lax.all_to_all(portions, "dp", split_axis=0, concat_axis=0, tiled=True)


def land(arranged, shape):
    landed = lax.all_to_all(arranged, "dp", split_axis=0, concat_axis=0, tiled=True)
    return landed.reshape(shape)


def body(qkv, gate, cotangent, out_weight, clip_lengths, text_lengths, plan):
    groups = lax.axis_size("dp")
    group_index = lax.axis_index("dp")
    seq_index = lax.axis_index("seq")
    core = seq_index & 1
    z_place = 2 * (group_index & 1) + (seq_index >> 1)
    ordinal = jnp.arange(groups, dtype=jnp.int32)
    inverse = jnp.sum(jnp.where(plan[None, :] == ordinal[:, None], ordinal[None, :], 0), axis=1)

    quarters = seq_index ^ jnp.arange(4, dtype=jnp.int32)
    text = lax.dynamic_slice_in_dim(text_lengths, 2 * group_index, 2)[:, None]
    video = lax.dynamic_slice_in_dim(clip_lengths, 2 * group_index, 2)[:, None]
    limits = jnp.where(quarters[None] == 0, text, video - (quarters[None] - 1) * ROWS)
    place = jnp.stack([core, z_place]).astype(jnp.int32)[:, None]
    plane = jnp.stack([group_index >> 3, (group_index >> 1) & 3]).astype(jnp.int32)[:, None]
    sp = jnp.concatenate([place, limits.astype(jnp.int32), plane], axis=1)
    first = core == 0

    def to_core(rows):
        other = jnp.where(first, rows[:, HALF:], rows[:, :HALF])
        return swap(other[None], 1)

    received = [None, None]
    d_own, d_peer = [None, None], [None, None]
    att, lse = [None, None], [None, None]

    cp = core.astype(jnp.int32).reshape(1, 1)
    send_1, keep_1, away = scaled_rows(cp, 1, cotangent, gate, out_weight)
    d_spread = spread_out(away)
    s1, s2, s3 = prep(after(cp, away), qkv, 1)
    received[1] = (swap(s1, 1), swap(s2, 2), swap(s3, 3))
    send_0, keep_0, near = scaled_rows(after(cp, s2), 0, cotangent, gate, out_weight)
    d_own[0], d_peer[0] = near[None], to_core(near)
    scaled = (keep_0, swap(send_0, 1), keep_1, swap(send_1, 1))
    d_picked = pick(d_spread, after(plan, near))
    landed = land(d_picked, (ROWS, WIDTH))
    s1, s2, s3 = prep(after(cp, d_picked), qkv, 0)
    received[0] = (swap(s1, 1), swap(s2, 2), swap(s3, 3))
    sp = after(sp, s2)
    att[1], lse[1] = attend(sp, 1, qkv, received[1])
    d_own[1], d_peer[1] = landed[None], to_core(landed)
    att_spread = spread_out(after(att[1], landed).reshape(2 * ROWS, HALF))

    def back(sp, slot):
        return attend_back(
            sp, slot, qkv, received[slot], att[slot], lse[slot], d_own[slot], d_peer[slot]
        )

    own_1, r1, r2, r3 = back(sp, 1)
    pieces_1 = (swap(r1, 1), swap(r3, 3))
    pieces_1 = (pieces_1[0], swap(r2, 2), pieces_1[1])
    att[0], lse[0] = attend(after(sp, r2), 0, qkv, received[0])
    att_other = [swap(att[0], 1)]
    picked = pick(att_spread, after(inverse, lse[0]))
    moved = land(picked, (2, ROWS, HALF))
    own_0, *sent_0 = back(after(sp, picked), 0)
    pieces_0 = [swap(rows, 1 + i) for i, rows in enumerate(sent_0)]
    balanced = [att[0], moved]
    att_other.append(swap(moved, 1))
    *partial, = weigh(after(sp, sent_0[1]), scaled, balanced, att_other)
    by_x, by_y = partial[:4], partial[4:]
    for step in (2, 1, 3):
        by_x[step] = along_x(by_x[step], step)
        by_y[step] = along_y(by_y[step], step)
    mixed, gate_part = project(
        after(sp, partial[0]), balanced, att_other, out_weight, gate, cotangent
    )
    gate_grad = gate_part + swap(gate_part, 1) + swap(gate_part, 2) + swap(gate_part, 3)
    grads = join(after(sp, gate_part), 1, own_1, *pieces_1, None)
    parts = list(sum_parts(after(sp, grads), by_x, by_y))
    low = parts[:1] + [along_y(parts[step], step) for step in (1, 2, 3)]
    high = parts[4:5] + [along_x(parts[4 + step], step) for step in (1, 2, 3)]
    grads = join(after(sp, parts[0]), 0, own_0, *pieces_0, grads)
    quarters = sum_weights(after(sp, grads), low, high)
    weight_grad = finish_weights(quarters)
    return (mixed, gate_grad, weight_grad, grads)


def solution(mesh):
    in_specs = (P("dp", "seq", None), P("dp", None), P("dp", "seq", None), P(), P(), P(), P())
    out_specs = (P("dp", "seq", None), P("dp", None), P(None, ("dp", "seq")), P("dp", "seq", None))
    return jax.shard_map(body, mesh=mesh, in_specs=in_specs, out_specs=out_specs, check_vma=False)
```

```python
import functools

import jax
import jax.numpy as jnp
from jax import lax
from jax.experimental import pallas as pl
from jax.experimental.pallas import tpu as pltpu
from jax.sharding import PartitionSpec as P


HD = 128
ROWS = 256
HEADS_HALF = 6
HALF = HEADS_HALF * HD
WIDTH = 2 * HALF
TOGETHER = 2
TOGETHER_BACK = 2
SHARE = 96
D = 3072
NEGATIVE = -1e30
LOG2E = 1.4426950408889634
SCALE = HD**-0.5

NT = (((1,), (1,)), ((), ()))
NN = (((1,), (0,)), ((), ()))
TN = (((0,), (0,)), ((), ()))


def mm(a, b, dims):
    return lax.dot_general(a, b, dims, preferred_element_type=jnp.float32)


def cost(flops, nbytes, transcendentals=0):
    return pl.CostEstimate(
        flops=int(flops), bytes_accessed=int(nbytes), transcendentals=int(transcendentals)
    )


def swap(x, step):
    return lax.ppermute(x, "seq", [(i, i ^ step) for i in range(4)])


def prep_kernel(sp, qo, ko, vo, kc, vc, s1, s2, s3):
    s1[0] = qo[0]
    s1[1] = ko[0]
    s1[2] = vo[0]
    s2[0] = kc[0]
    s2[1] = vc[0]
    s3[0] = ko[0]
    s3[1] = vo[0]


def prep(sp, qkv, slot):
    rows = ROWS // 2

    def half(member, other):
        def index(r, sp):
            core = sp[0, 0]
            return (slot, r, 2 * member + (1 - core if other else core))

        return pl.BlockSpec((1, rows, HALF), index)

    def out(count):
        return pl.BlockSpec((count, rows, HALF), lambda r, sp: (0, r, 0))

    def shape(count):
        return jax.ShapeDtypeStruct((count, ROWS, HALF), jnp.bfloat16)

    return pl.pallas_call(
        prep_kernel,
        grid_spec=pltpu.PrefetchScalarGridSpec(
            num_scalar_prefetch=1,
            grid=(2,),
            in_specs=[half(0, True), half(1, True), half(2, True), half(1, False), half(2, False)],
            out_specs=[out(3), out(2), out(2)],
        ),
        out_shape=[shape(3), shape(2), shape(2)],
        cost_estimate=cost(1e6, 5e6),
    )(sp, qkv, qkv, qkv, qkv, qkv)


def live_limit(sp, slot, block, shape, axis):
    return lax.broadcasted_iota(jnp.int32, shape, axis) < sp[slot, 1 + block]


def key_bias(sp, slot, axis):
    shape = (ROWS, 1) if axis == 0 else (1, ROWS)
    parts = [
        jnp.where(live_limit(sp, slot, block, shape, axis), 0.0, NEGATIVE) for block in range(4)
    ]
    return jnp.concatenate(parts, axis=axis)


def fwd_kernel(slot, sp, q0, k0, v0, q1, k1, v1, k2, v2, k3, v3, att, lse):
    bias = key_bias(sp, slot, 1)
    work = []
    for head in range(TOGETHER):
        cols = slice(head * HD, (head + 1) * HD)
        keys = jnp.concatenate([k[0, :, cols] for k in (k0, k1, k2, k3)], axis=0)
        values = jnp.concatenate([v[0, :, cols] for v in (v0, v1, v2, v3)], axis=0)
        for block, q in enumerate((q0, q1)):
            work.append((head, cols, block, mm(q[0, :, cols], keys, NT), values))
    for head, cols, block, products, values in work:
        scores = products * (SCALE * LOG2E) + bias
        peak = jnp.max(scores, axis=1, keepdims=True)
        powers = jnp.exp2(scores - peak)
        total = jnp.sum(powers, axis=1, keepdims=True)
        live = live_limit(sp, slot, block, (ROWS, 1), 0)
        inverse = jnp.where(live, 1.0 / total, 0.0)
        mixed = mm(powers.astype(jnp.bfloat16), values, NN) * inverse
        att[block, :, cols] = mixed.astype(jnp.bfloat16)
        level = jnp.where(live, peak + jnp.log2(total), -NEGATIVE)
        lse[head, :, block * ROWS : (block + 1) * ROWS] = jnp.broadcast_to(level, (ROWS, HD)).T[:8]


def bwd_kernel(
    slot, sp, q0, k0, v0, q1, k1, v1, k2, v2, k3, v3, att, lse, do0, do1, own, r1, r2, r3
):
    bias = key_bias(sp, slot, 0)
    low = jnp.bfloat16
    for head in range(TOGETHER_BACK):
        cols = slice(head * HD, (head + 1) * HD)
        keys = jnp.concatenate([k[0, :, cols] for k in (k0, k1, k2, k3)], axis=0)
        values = jnp.concatenate([v[0, :, cols] for v in (v0, v1, v2, v3)], axis=0)
        grad_k = None
        grad_v = None
        for block, (q, do) in enumerate(((q0, do0), (q1, do1))):
            q_rows = q[0, :, cols]
            d_rows = do[0, :, cols]
            scores = mm(keys, q_rows, NT) * (SCALE * LOG2E) + bias
            level = lse[head, 0:1, block * ROWS : (block + 1) * ROWS]
            probs = jnp.exp2(scores - level)
            product = d_rows.astype(jnp.float32) * att[block, :, cols].astype(jnp.float32)
            dots = jnp.sum(product.T, axis=0, keepdims=True)
            d_probs = mm(values, d_rows, NT)
            d_scores = (probs * (d_probs - dots)).astype(low)
            v_part = mm(probs.astype(low), d_rows, NN)
            k_part = mm(d_scores, q_rows, NN)
            grad_k = k_part if block == 0 else grad_k + k_part
            grad_v = v_part if block == 0 else grad_v + v_part
            grad_q = (mm(keys, d_scores, TN) * SCALE).T
            if block == 0:
                own[0, :, cols] = grad_q
            else:
                r1[0, :, cols] = grad_q.astype(low)
        grad_k = grad_k * SCALE
        own[1, :, cols] = grad_k[:ROWS]
        own[2, :, cols] = grad_v[:ROWS]
        r1[1, :, cols] = grad_k[ROWS : 2 * ROWS].astype(low)
        r1[2, :, cols] = grad_v[ROWS : 2 * ROWS].astype(low)
        r2[0, :, cols] = grad_k[2 * ROWS : 3 * ROWS].astype(low)
        r2[1, :, cols] = grad_v[2 * ROWS : 3 * ROWS].astype(low)
        r3[0, :, cols] = grad_k[3 * ROWS :].astype(low)
        r3[1, :, cols] = grad_v[3 * ROWS :].astype(low)


def head_block(lead, index=0, heads=1):
    return pl.BlockSpec((lead, ROWS, heads * HD), lambda h, sp: (index, 0, h))


def section_specs(slot, heads=1):
    def own(member):
        return pl.BlockSpec(
            (1, ROWS, heads * HD),
            lambda h, sp: (slot, 0, (12 * member + HEADS_HALF * sp[0, 0]) // heads + h),
        )

    return [own(0), own(1), own(2)] + [head_block(1, m, heads) for m in (0, 1, 2, 0, 1, 0, 1)]


def sections(qkv, x1, x2, x3):
    return (qkv, qkv, qkv, x1, x1, x1, x2, x2, x3, x3)


PAIRS = HEADS_HALF * 512 * 1024


def attend(sp, slot, qkv, received):
    return pl.pallas_call(
        functools.partial(fwd_kernel, slot),
        grid_spec=pltpu.PrefetchScalarGridSpec(
            num_scalar_prefetch=1,
            grid=(HEADS_HALF // TOGETHER,),
            in_specs=section_specs(slot, TOGETHER),
            out_specs=[
                head_block(2, 0, TOGETHER),
                pl.BlockSpec((TOGETHER, 8, 2 * ROWS), lambda h, sp: (h, 0, 0)),
            ],
        ),
        out_shape=[
            jax.ShapeDtypeStruct((2, ROWS, HALF), jnp.bfloat16),
            jax.ShapeDtypeStruct((HEADS_HALF, 8, 2 * ROWS), jnp.float32),
        ],
        cost_estimate=cost(4 * PAIRS * HD, 5e6, PAIRS),
    )(sp, *sections(qkv, *received))


def attend_back(sp, slot, qkv, received, att, lse, d_own, d_peer):
    heads = TOGETHER_BACK
    d_own_spec = pl.BlockSpec(
        (1, ROWS, heads * HD), lambda h, sp: (0, 0, HEADS_HALF // heads * sp[0, 0] + h)
    )

    def shape(count, kind):
        return jax.ShapeDtypeStruct((count, ROWS, HALF), kind)

    def piece(count):
        return head_block(count, 0, heads)

    return pl.pallas_call(
        functools.partial(bwd_kernel, slot),
        grid_spec=pltpu.PrefetchScalarGridSpec(
            num_scalar_prefetch=1,
            grid=(HEADS_HALF // heads,),
            in_specs=section_specs(slot, heads)
            + [
                piece(2),
                pl.BlockSpec((heads, 8, 2 * ROWS), lambda h, sp: (h, 0, 0)),
                d_own_spec,
                piece(1),
            ],
            out_specs=[piece(3), piece(3), piece(2), piece(2)],
        ),
        out_shape=[
            shape(3, jnp.float32),
            shape(3, jnp.bfloat16),
            shape(2, jnp.bfloat16),
            shape(2, jnp.bfloat16),
        ],
        cost_estimate=cost(10 * PAIRS * HD, 1e7, PAIRS),
    )(sp, *sections(qkv, *received), att, lse, d_own, d_peer)


def join_kernel(sp, own, p1, p2, p3, *rest):
    out = rest[-1]
    core = sp[0, 0]
    member = pl.program_id(0)
    crossing = jnp.where(member > 0, 1.0, 0.0)
    mine = own[0] + crossing * p2[0].astype(jnp.float32)
    other = p1[0].astype(jnp.float32) + crossing * p3[0].astype(jnp.float32)
    first = core == 0
    out[0, :, :HALF] = jnp.where(first, mine, other).astype(jnp.bfloat16)
    out[0, :, HALF:] = jnp.where(first, other, mine).astype(jnp.bfloat16)


def join(sp, slot, own, p1, p2, p3, base):
    def piece(shift):
        return pl.BlockSpec((1, ROWS, HALF), lambda m, sp: (jnp.maximum(m - shift, 0), 0, 0))

    in_specs = [piece(0), piece(0), piece(1), piece(1)]
    args = [own, p1, p2, p3]
    aliases = {}
    if base is not None:
        in_specs.append(pl.BlockSpec(memory_space=pl.ANY))
        args.append(base)
        aliases = {5: 0}
    return pl.pallas_call(
        join_kernel,
        grid_spec=pltpu.PrefetchScalarGridSpec(
            num_scalar_prefetch=1,
            grid=(3,),
            in_specs=in_specs,
            out_specs=pl.BlockSpec((1, ROWS, WIDTH), lambda m, sp: (slot, 0, m)),
        ),
        out_shape=jax.ShapeDtypeStruct((2, ROWS, 3 * WIDTH), jnp.bfloat16),
        input_output_aliases=aliases,
        cost_estimate=cost(1e6, 1e7),
    )(sp, *args)


def pick_kernel(order, rows, out):
    def step(slot, carry):
        out[slot] = rows[order[slot]]
        return carry

    lax.fori_loop(0, rows.shape[0], step, 0)


def pick(rows, order):
    whole = pl.BlockSpec(rows.shape, lambda i, order: (0, 0, 0))
    return pl.pallas_call(
        pick_kernel,
        grid_spec=pltpu.PrefetchScalarGridSpec(
            num_scalar_prefetch=1, grid=(1,), in_specs=[whole], out_specs=whole
        ),
        out_shape=jax.ShapeDtypeStruct(rows.shape, rows.dtype),
        cost_estimate=cost(1e6, 2 * rows.size * 2),
        name="pick",
    )(order, rows)


def rows_kernel(slot, sp, cotangent, gate, weight, send, keep, rows, total):
    step = pl.program_id(0)
    scaled = (cotangent[0].astype(jnp.float32) * gate[slot : slot + 1]).astype(jnp.bfloat16)

    @pl.when(step < 2)
    def _():
        send[...] = scaled

    @pl.when(step >= 2)
    def _():
        keep[...] = scaled

    product = mm(scaled, weight[...], NT)

    @pl.when(step == 0)
    def _():
        total[...] = product

    @pl.when((step > 0) & (step < 3))
    def _():
        total[...] += product

    @pl.when(step == 3)
    def _():
        rows[...] = (total[...] + product).astype(jnp.bfloat16)


def scaled_rows(sp, slot, cotangent, gate, out_weight):
    cols = D // 4

    def place(step, sp):
        core = sp[0, 0]
        return jnp.where(step < 2, 2 * (1 - core), 2 * core - 2) + step

    def shape(cols):
        return jax.ShapeDtypeStruct((ROWS, cols), jnp.bfloat16)

    return pl.pallas_call(
        functools.partial(rows_kernel, slot),
        grid_spec=pltpu.PrefetchScalarGridSpec(
            num_scalar_prefetch=1,
            grid=(4,),
            in_specs=[
                pl.BlockSpec((1, ROWS, cols), lambda k, sp: (slot, 0, place(k, sp))),
                pl.BlockSpec((2, cols), lambda k, sp: (0, place(k, sp))),
                pl.BlockSpec((WIDTH, cols), lambda k, sp: (0, place(k, sp))),
            ],
            out_specs=[
                pl.BlockSpec((ROWS, cols), lambda k, sp: (0, jnp.minimum(k, 1))),
                pl.BlockSpec((ROWS, cols), lambda k, sp: (0, jnp.maximum(k - 2, 0))),
                pl.BlockSpec((ROWS, WIDTH), lambda k, sp: (0, 0)),
            ],
            scratch_shapes=[pltpu.VMEM((ROWS, WIDTH), jnp.float32)],
        ),
        out_shape=[shape(D // 2), shape(D // 2), shape(WIDTH)],
        cost_estimate=cost(2 * 256 * WIDTH * D, 1.3e7),
    )(sp, cotangent, gate, out_weight)


def project_kernel(sp, a0, a1, b0, b1, w_mine, w_other, gate, cotangent, mixed, gate_grad):
    mine = jnp.concatenate([a0[0], a1[0]], axis=0)
    other = jnp.concatenate([b0[0], b1[0]], axis=0)
    outputs = mm(mine, w_mine[...], NN) + mm(other, w_other[...], NN)
    for slot in range(2):
        rows = outputs[slot * ROWS : (slot + 1) * ROWS]
        mixed[slot] = (rows * gate[slot : slot + 1]).astype(jnp.bfloat16)
        gate_grad[slot : slot + 1] = jnp.sum(
            cotangent[slot].astype(jnp.float32) * rows, axis=0, keepdims=True
        )


def project(sp, mine, other, out_weight, gate, cotangent):
    cols = 1024

    def rows(index):
        return pl.BlockSpec((1, ROWS, HALF), lambda d, sp: (index, 0, 0))

    wide = pl.BlockSpec((2, ROWS, cols), lambda d, sp: (0, 0, d))
    thin = pl.BlockSpec((2, cols), lambda d, sp: (0, d))
    return pl.pallas_call(
        project_kernel,
        grid_spec=pltpu.PrefetchScalarGridSpec(
            num_scalar_prefetch=1,
            grid=(D // cols,),
            in_specs=[
                rows(0),
                rows(0),
                rows(1),
                rows(1),
                pl.BlockSpec((HALF, cols), lambda d, sp: (sp[0, 0], d)),
                pl.BlockSpec((HALF, cols), lambda d, sp: (1 - sp[0, 0], d)),
                thin,
                wide,
            ],
            out_specs=[wide, thin],
        ),
        out_shape=[
            jax.ShapeDtypeStruct((2, ROWS, D), jnp.bfloat16),
            jax.ShapeDtypeStruct((2, D), jnp.float32),
        ],
        cost_estimate=cost(2 * 512 * WIDTH * D, 1.6e7),
        name="project",
    )(sp, mine[0], mine[1], other[0], other[1], out_weight, out_weight, gate, cotangent)


def weigh_kernel(sp, own0, peer0, own1, peer1, a0, a1, b0, b1, *rest):
    outs, product = rest[:8], rest[8]
    step = pl.program_id(0)
    left = jnp.concatenate([own0[...], peer0[...], own1[...], peer1[...]], axis=0)
    mine = jnp.concatenate([a0[0], a0[1], a1[0], a1[1]], axis=0)
    other = jnp.concatenate([b0[1], b0[0], b1[1], b1[0]], axis=0)
    by_x = mm(left, mine, TN).astype(jnp.bfloat16)
    for x_step in range(4):

        @pl.when(step == x_step)
        def _():
            outs[x_step][...] = by_x

    product[...] = mm(left, other, TN)
    for y_step in range(4):
        start = pl.multiple_of((sp[1, 5] ^ y_step) * SHARE, 8)
        rows = product[pl.ds(start, SHARE), :].astype(jnp.bfloat16)
        outs[4 + y_step][sp[0, 5] ^ step] = rows


def weigh(sp, scaled, mine, other):
    rows = D // 8
    pair = pl.BlockSpec((2, ROWS, HALF), lambda d, sp: (0, 0, 0))
    wide = pl.BlockSpec((ROWS, rows), lambda d, sp: (0, sp[0, 5] ^ d))
    return pl.pallas_call(
        weigh_kernel,
        grid_spec=pltpu.PrefetchScalarGridSpec(
            num_scalar_prefetch=1,
            grid=(4,),
            in_specs=[wide] * 4 + [pair] * 4,
            out_specs=[pl.BlockSpec((rows, HALF), lambda d, sp: (0, 0))] * 4
            + [pl.BlockSpec((4, SHARE, HALF), lambda d, sp: (0, 0, 0))] * 4,
            scratch_shapes=[pltpu.VMEM((rows, HALF), jnp.float32)],
        ),
        out_shape=[jax.ShapeDtypeStruct((rows, HALF), jnp.bfloat16)] * 4
        + [jax.ShapeDtypeStruct((4, SHARE, HALF), jnp.bfloat16)] * 4,
        cost_estimate=cost(2 * 1024 * WIDTH * D // 2, 1.2e7),
        name="weigh",
    )(sp, *scaled, mine[0], mine[1], other[0], other[1])


def along_x(x, step):
    return lax.ppermute(x, "dp", [(g, g ^ (step << 3)) for g in range(32)])


def along_y(x, step):
    return lax.ppermute(x, "dp", [(g, g ^ (step << 1)) for g in range(32)])


def add_up(refs):
    total = refs[0][...].astype(jnp.float32)
    for ref in refs[1:]:
        total = total + ref[...].astype(jnp.float32)
    return total


def part_kernel(sp, *refs):
    by_x, by_y, outs, total = refs[:4], refs[4:8], refs[8:16], refs[16]
    total[...] = add_up(by_x)
    for step in range(4):
        start = pl.multiple_of((sp[1, 5] ^ step) * SHARE, 8)
        outs[step][...] = total[pl.ds(start, SHARE), :].astype(jnp.bfloat16)
    for step in range(4):
        place = sp[0, 5] ^ step
        rows = by_y[0][place].astype(jnp.float32)
        for ref in by_y[1:]:
            rows = rows + ref[place].astype(jnp.float32)
        outs[4 + step][...] = rows.astype(jnp.bfloat16)


def sum_parts(sp, by_x, by_y):
    cols = HALF // 2
    share = pl.BlockSpec((SHARE, cols), lambda i, sp: (0, i))
    return pl.pallas_call(
        part_kernel,
        grid_spec=pltpu.PrefetchScalarGridSpec(
            num_scalar_prefetch=1,
            grid=(2,),
            in_specs=[pl.BlockSpec((4 * SHARE, cols), lambda i, sp: (0, i))] * 4
            + [pl.BlockSpec((4, SHARE, cols), lambda i, sp: (0, 0, i))] * 4,
            out_specs=[share] * 8,
            scratch_shapes=[pltpu.VMEM((4 * SHARE, cols), jnp.float32)],
        ),
        out_shape=[jax.ShapeDtypeStruct((SHARE, HALF), jnp.bfloat16)] * 8,
        cost_estimate=cost(5e6, 6e6),
        name="sum_parts",
    )(sp, *by_x, *by_y)


def final_moves(step):
    moves = []
    for xy in range(16):
        for z_low in range(2):
            for z_high in range(2):
                for core in range(2):
                    source = 4 * (2 * xy + z_low) + 2 * z_high + core
                    target = 4 * (16 * core + xy) + ((2 * z_low + z_high) ^ step)
                    moves.append((source, target))
    return moves


def sum_kernel(sp, *refs):
    low, high, outs, total = refs[:4], refs[4:8], refs[8:12], refs[12]
    first = sp[0, 0] == 0
    mine = add_up(low)
    other = add_up(high)
    total[:, :HALF] = jnp.where(first, mine, other)
    total[:, HALF:] = jnp.where(first, other, mine)
    count = SHARE // 4
    for step, out in enumerate(outs):
        start = pl.multiple_of((sp[1, 0] ^ step) * count, 8)
        out[...] = total[pl.ds(start, count), :].astype(jnp.bfloat16)


def sum_weights(sp, low, high):
    def whole(rows, cols):
        return pl.BlockSpec((rows, cols), lambda i, sp: (0, 0))

    return pl.pallas_call(
        sum_kernel,
        grid_spec=pltpu.PrefetchScalarGridSpec(
            num_scalar_prefetch=1,
            grid=(1,),
            in_specs=[whole(SHARE, HALF)] * 8,
            out_specs=[whole(SHARE // 4, WIDTH)] * 4,
            scratch_shapes=[pltpu.VMEM((SHARE, WIDTH), jnp.float32)],
        ),
        out_shape=[jax.ShapeDtypeStruct((SHARE // 4, WIDTH), jnp.bfloat16)] * 4,
        cost_estimate=cost(1e6, 2e6),
        name="sum_weights",
    )(sp, *low, *high)


def finish_weights(quarters):
    pieces = [
        lax.ppermute(quarter, ("dp", "seq"), final_moves(step)).astype(jnp.float32)
        for step, quarter in enumerate(quarters)
    ]
    return (pieces[0] + pieces[1] + pieces[2] + pieces[3]).T


def after(value, *others):
    return lax.optimization_barrier((value, *others))[0]


def spread_out(rows):
    groups = lax.axis_size("dp")
    portions = rows.reshape(groups, -1, rows.shape[-1])
    return lax.all_to_all(portions, "dp", split_axis=0, concat_axis=0, tiled=True)


def land(arranged, shape):
    landed = lax.all_to_all(arranged, "dp", split_axis=0, concat_axis=0, tiled=True)
    return landed.reshape(shape)


def body(qkv, gate, cotangent, out_weight, clip_lengths, text_lengths, plan):
    groups = lax.axis_size("dp")
    group_index = lax.axis_index("dp")
    seq_index = lax.axis_index("seq")
    core = seq_index & 1
    z_place = 2 * (group_index & 1) + (seq_index >> 1)
    ordinal = jnp.arange(groups, dtype=jnp.int32)
    inverse = jnp.sum(jnp.where(plan[None, :] == ordinal[:, None], ordinal[None, :], 0), axis=1)

    quarters = seq_index ^ jnp.arange(4, dtype=jnp.int32)
    text = lax.dynamic_slice_in_dim(text_lengths, 2 * group_index, 2)[:, None]
    video = lax.dynamic_slice_in_dim(clip_lengths, 2 * group_index, 2)[:, None]
    limits = jnp.where(quarters[None] == 0, text, video - (quarters[None] - 1) * ROWS)
    place = jnp.stack([core, z_place]).astype(jnp.int32)[:, None]
    plane = jnp.stack([group_index >> 3, (group_index >> 1) & 3]).astype(jnp.int32)[:, None]
    sp = jnp.concatenate([place, limits.astype(jnp.int32), plane], axis=1)
    first = core == 0

    def to_core(rows):
        other = jnp.where(first, rows[:, HALF:], rows[:, :HALF])
        return swap(other[None], 1)

    received = [None, None]
    d_own, d_peer = [None, None], [None, None]
    att, lse = [None, None], [None, None]

    cp = core.astype(jnp.int32).reshape(1, 1)
    s1, s2, s3 = prep(cp, qkv, 1)
    received[1] = (swap(s1, 1), swap(s2, 2), swap(s3, 3))
    send_1, keep_1, away = scaled_rows(after(cp, s2), 1, cotangent, gate, out_weight)
    d_spread = spread_out(away)
    s1, s2, s3 = prep(after(cp, away), qkv, 0)
    near_keys = (swap(s1, 1), swap(s3, 3))
    received[0] = (near_keys[0], swap(s2, 2), near_keys[1])
    send_0, keep_0, near = scaled_rows(after(cp, s2), 0, cotangent, gate, out_weight)
    d_own[0], d_peer[0] = near[None], to_core(near)
    scaled = (keep_0, swap(send_0, 1), keep_1, swap(send_1, 1))
    d_picked = pick(d_spread, after(plan, near))
    landed = land(d_picked, (ROWS, WIDTH))
    sp = after(sp, d_picked)
    att[1], lse[1] = attend(sp, 1, qkv, received[1])
    d_own[1], d_peer[1] = landed[None], to_core(landed)
    att_spread = spread_out(after(att[1], landed).reshape(2 * ROWS, HALF))

    def back(sp, slot):
        return attend_back(
            sp, slot, qkv, received[slot], att[slot], lse[slot], d_own[slot], d_peer[slot]
        )

    own_1, r1, r2, r3 = back(sp, 1)
    pieces_1 = (swap(r1, 1), swap(r3, 3))
    pieces_1 = (pieces_1[0], swap(r2, 2), pieces_1[1])
    att[0], lse[0] = attend(after(sp, r2), 0, qkv, received[0])
    att_other = [swap(att[0], 1)]
    picked = pick(att_spread, after(inverse, lse[0]))
    moved = land(picked, (2, ROWS, HALF))
    own_0, *sent_0 = back(after(sp, picked), 0)
    pieces_0 = [swap(rows, 1 + i) for i, rows in enumerate(sent_0)]
    balanced = [att[0], moved]
    att_other.append(swap(moved, 1))
    *partial, = weigh(after(sp, sent_0[1]), scaled, balanced, att_other)
    by_x, by_y = partial[:4], partial[4:]
    for step in (2, 1, 3):
        by_x[step] = along_x(by_x[step], step)
        by_y[step] = along_y(by_y[step], step)
    mixed, gate_part = project(
        after(sp, partial[0]), balanced, att_other, out_weight, gate, cotangent
    )
    gate_grad = gate_part + swap(gate_part, 1) + swap(gate_part, 2) + swap(gate_part, 3)
    grads = join(after(sp, gate_part), 1, own_1, *pieces_1, None)
    parts = list(sum_parts(after(sp, grads), by_x, by_y))
    low = parts[:1] + [along_y(parts[step], step) for step in (1, 2, 3)]
    high = parts[4:5] + [along_x(parts[4 + step], step) for step in (1, 2, 3)]
    grads = join(after(sp, parts[0]), 0, own_0, *pieces_0, grads)
    quarters = sum_weights(after(sp, grads), low, high)
    weight_grad = finish_weights(quarters)
    return (mixed, gate_grad, weight_grad, grads)


def solution(mesh):
    in_specs = (P("dp", "seq", None), P("dp", None), P("dp", "seq", None), P(), P(), P(), P())
    out_specs = (P("dp", "seq", None), P("dp", None), P(None, ("dp", "seq")), P("dp", "seq", None))
    return jax.shard_map(body, mesh=mesh, in_specs=in_specs, out_specs=out_specs, check_vma=False)
```

```python
import functools

import jax
import jax.numpy as jnp
from jax import lax
from jax.experimental import pallas as pl
from jax.experimental.pallas import tpu as pltpu
from jax.sharding import PartitionSpec as P


HD = 128
ROWS = 256
HEADS_HALF = 6
HALF = HEADS_HALF * HD
WIDTH = 2 * HALF
TOGETHER = 2
TOGETHER_BACK = 2
SHARE = 96
D = 3072
NEGATIVE = -1e30
LOG2E = 1.4426950408889634
SCALE = HD**-0.5

NT = (((1,), (1,)), ((), ()))
NN = (((1,), (0,)), ((), ()))
TN = (((0,), (0,)), ((), ()))


def mm(a, b, dims):
    return lax.dot_general(a, b, dims, preferred_element_type=jnp.float32)


def cost(flops, nbytes, transcendentals=0):
    return pl.CostEstimate(
        flops=int(flops), bytes_accessed=int(nbytes), transcendentals=int(transcendentals)
    )


def swap(x, step):
    return lax.ppermute(x, "seq", [(i, i ^ step) for i in range(4)])


def prep_kernel(sp, qo, ko, vo, kc, vc, s1, s2, s3):
    s1[0] = qo[0]
    s1[1] = ko[0]
    s1[2] = vo[0]
    s2[0] = kc[0]
    s2[1] = vc[0]
    s3[0] = ko[0]
    s3[1] = vo[0]


def prep(sp, qkv, slot):
    rows = ROWS // 2

    def half(member, other):
        def index(r, sp):
            core = sp[0, 0]
            return (slot, r, 2 * member + (1 - core if other else core))

        return pl.BlockSpec((1, rows, HALF), index)

    def out(count):
        return pl.BlockSpec((count, rows, HALF), lambda r, sp: (0, r, 0))

    def shape(count):
        return jax.ShapeDtypeStruct((count, ROWS, HALF), jnp.bfloat16)

    return pl.pallas_call(
        prep_kernel,
        grid_spec=pltpu.PrefetchScalarGridSpec(
            num_scalar_prefetch=1,
            grid=(2,),
            in_specs=[half(0, True), half(1, True), half(2, True), half(1, False), half(2, False)],
            out_specs=[out(3), out(2), out(2)],
        ),
        out_shape=[shape(3), shape(2), shape(2)],
        cost_estimate=cost(1e6, 5e6),
    )(sp, qkv, qkv, qkv, qkv, qkv)


def live_limit(sp, slot, block, shape, axis):
    return lax.broadcasted_iota(jnp.int32, shape, axis) < sp[slot, 1 + block]


def key_bias(sp, slot, axis):
    shape = (ROWS, 1) if axis == 0 else (1, ROWS)
    parts = [
        jnp.where(live_limit(sp, slot, block, shape, axis), 0.0, NEGATIVE) for block in range(4)
    ]
    return jnp.concatenate(parts, axis=axis)


def fwd_kernel(slot, sp, q0, k0, v0, q1, k1, v1, k2, v2, k3, v3, att, lse):
    bias = key_bias(sp, slot, 1)
    work = []
    for head in range(TOGETHER):
        cols = slice(head * HD, (head + 1) * HD)
        keys = jnp.concatenate([k[0, :, cols] for k in (k0, k1, k2, k3)], axis=0)
        values = jnp.concatenate([v[0, :, cols] for v in (v0, v1, v2, v3)], axis=0)
        for block, q in enumerate((q0, q1)):
            work.append((head, cols, block, mm(q[0, :, cols], keys, NT), values))
    for head, cols, block, products, values in work:
        scores = products * (SCALE * LOG2E) + bias
        peak = jnp.max(scores, axis=1, keepdims=True)
        powers = jnp.exp2(scores - peak)
        total = jnp.sum(powers, axis=1, keepdims=True)
        live = live_limit(sp, slot, block, (ROWS, 1), 0)
        inverse = jnp.where(live, 1.0 / total, 0.0)
        mixed = mm(powers.astype(jnp.bfloat16), values, NN) * inverse
        att[block, :, cols] = mixed.astype(jnp.bfloat16)
        level = jnp.where(live, peak + jnp.log2(total), -NEGATIVE)
        lse[head, :, block * ROWS : (block + 1) * ROWS] = jnp.broadcast_to(level, (ROWS, HD)).T[:8]


def bwd_kernel(
    slot, sp, q0, k0, v0, q1, k1, v1, k2, v2, k3, v3, att, lse, do0, do1, own, r1, r2, r3
):
    bias = key_bias(sp, slot, 0)
    low = jnp.bfloat16
    for head in range(TOGETHER_BACK):
        cols = slice(head * HD, (head + 1) * HD)
        keys = jnp.concatenate([k[0, :, cols] for k in (k0, k1, k2, k3)], axis=0)
        values = jnp.concatenate([v[0, :, cols] for v in (v0, v1, v2, v3)], axis=0)
        grad_k = None
        grad_v = None
        for block, (q, do) in enumerate(((q0, do0), (q1, do1))):
            q_rows = q[0, :, cols]
            d_rows = do[0, :, cols]
            scores = mm(keys, q_rows, NT) * (SCALE * LOG2E) + bias
            level = lse[head, 0:1, block * ROWS : (block + 1) * ROWS]
            probs = jnp.exp2(scores - level)
            product = d_rows.astype(jnp.float32) * att[block, :, cols].astype(jnp.float32)
            dots = jnp.sum(product.T, axis=0, keepdims=True)
            d_probs = mm(values, d_rows, NT)
            d_scores = (probs * (d_probs - dots)).astype(low)
            v_part = mm(probs.astype(low), d_rows, NN)
            k_part = mm(d_scores, q_rows, NN)
            grad_k = k_part if block == 0 else grad_k + k_part
            grad_v = v_part if block == 0 else grad_v + v_part
            grad_q = (mm(keys, d_scores, TN) * SCALE).T
            if block == 0:
                own[0, :, cols] = grad_q
            else:
                r1[0, :, cols] = grad_q.astype(low)
        grad_k = grad_k * SCALE
        own[1, :, cols] = grad_k[:ROWS]
        own[2, :, cols] = grad_v[:ROWS]
        r1[1, :, cols] = grad_k[ROWS : 2 * ROWS].astype(low)
        r1[2, :, cols] = grad_v[ROWS : 2 * ROWS].astype(low)
        r2[0, :, cols] = grad_k[2 * ROWS : 3 * ROWS].astype(low)
        r2[1, :, cols] = grad_v[2 * ROWS : 3 * ROWS].astype(low)
        r3[0, :, cols] = grad_k[3 * ROWS :].astype(low)
        r3[1, :, cols] = grad_v[3 * ROWS :].astype(low)


def head_block(lead, index=0, heads=1):
    return pl.BlockSpec((lead, ROWS, heads * HD), lambda h, sp: (index, 0, h))


def section_specs(slot, heads=1):
    def own(member):
        return pl.BlockSpec(
            (1, ROWS, heads * HD),
            lambda h, sp: (slot, 0, (12 * member + HEADS_HALF * sp[0, 0]) // heads + h),
        )

    return [own(0), own(1), own(2)] + [head_block(1, m, heads) for m in (0, 1, 2, 0, 1, 0, 1)]


def sections(qkv, x1, x2, x3):
    return (qkv, qkv, qkv, x1, x1, x1, x2, x2, x3, x3)


PAIRS = HEADS_HALF * 512 * 1024


def attend(sp, slot, qkv, received):
    return pl.pallas_call(
        functools.partial(fwd_kernel, slot),
        grid_spec=pltpu.PrefetchScalarGridSpec(
            num_scalar_prefetch=1,
            grid=(HEADS_HALF // TOGETHER,),
            in_specs=section_specs(slot, TOGETHER),
            out_specs=[
                head_block(2, 0, TOGETHER),
                pl.BlockSpec((TOGETHER, 8, 2 * ROWS), lambda h, sp: (h, 0, 0)),
            ],
        ),
        out_shape=[
            jax.ShapeDtypeStruct((2, ROWS, HALF), jnp.bfloat16),
            jax.ShapeDtypeStruct((HEADS_HALF, 8, 2 * ROWS), jnp.float32),
        ],
        cost_estimate=cost(4 * PAIRS * HD, 5e6, PAIRS),
    )(sp, *sections(qkv, *received))


def attend_back(sp, slot, qkv, received, att, lse, d_own, d_peer):
    heads = TOGETHER_BACK
    d_own_spec = pl.BlockSpec(
        (1, ROWS, heads * HD), lambda h, sp: (0, 0, HEADS_HALF // heads * sp[0, 0] + h)
    )

    def shape(count, kind):
        return jax.ShapeDtypeStruct((count, ROWS, HALF), kind)

    def piece(count):
        return head_block(count, 0, heads)

    return pl.pallas_call(
        functools.partial(bwd_kernel, slot),
        grid_spec=pltpu.PrefetchScalarGridSpec(
            num_scalar_prefetch=1,
            grid=(HEADS_HALF // heads,),
            in_specs=section_specs(slot, heads)
            + [
                piece(2),
                pl.BlockSpec((heads, 8, 2 * ROWS), lambda h, sp: (h, 0, 0)),
                d_own_spec,
                d_own_spec,
            ],
            out_specs=[piece(3), piece(3), piece(2), piece(2)],
        ),
        out_shape=[
            shape(3, jnp.float32),
            shape(3, jnp.bfloat16),
            shape(2, jnp.bfloat16),
            shape(2, jnp.bfloat16),
        ],
        cost_estimate=cost(10 * PAIRS * HD, 1e7, PAIRS),
    )(sp, *sections(qkv, *received), att, lse, d_own, d_peer)


def join_kernel(sp, own, p1, p2, p3, *rest):
    out = rest[-1]
    core = sp[0, 0]
    member = pl.program_id(0)
    crossing = jnp.where(member > 0, 1.0, 0.0)
    mine = own[0] + crossing * p2[0].astype(jnp.float32)
    other = p1[0].astype(jnp.float32) + crossing * p3[0].astype(jnp.float32)
    first = core == 0
    out[0, :, :HALF] = jnp.where(first, mine, other).astype(jnp.bfloat16)
    out[0, :, HALF:] = jnp.where(first, other, mine).astype(jnp.bfloat16)


def join(sp, slot, own, p1, p2, p3, base):
    def piece(shift):
        return pl.BlockSpec((1, ROWS, HALF), lambda m, sp: (jnp.maximum(m - shift, 0), 0, 0))

    in_specs = [piece(0), piece(0), piece(1), piece(1)]
    args = [own, p1, p2, p3]
    aliases = {}
    if base is not None:
        in_specs.append(pl.BlockSpec(memory_space=pl.ANY))
        args.append(base)
        aliases = {5: 0}
    return pl.pallas_call(
        join_kernel,
        grid_spec=pltpu.PrefetchScalarGridSpec(
            num_scalar_prefetch=1,
            grid=(3,),
            in_specs=in_specs,
            out_specs=pl.BlockSpec((1, ROWS, WIDTH), lambda m, sp: (slot, 0, m)),
        ),
        out_shape=jax.ShapeDtypeStruct((2, ROWS, 3 * WIDTH), jnp.bfloat16),
        input_output_aliases=aliases,
        cost_estimate=cost(1e6, 1e7),
    )(sp, *args)


def pick_kernel(order, rows, out):
    def step(slot, carry):
        out[slot] = rows[order[slot]]
        return carry

    lax.fori_loop(0, rows.shape[0], step, 0)


def pick(rows, order):
    whole = pl.BlockSpec(rows.shape, lambda i, order: (0, 0, 0))
    return pl.pallas_call(
        pick_kernel,
        grid_spec=pltpu.PrefetchScalarGridSpec(
            num_scalar_prefetch=1, grid=(1,), in_specs=[whole], out_specs=whole
        ),
        out_shape=jax.ShapeDtypeStruct(rows.shape, rows.dtype),
        cost_estimate=cost(1e6, 2 * rows.size * 2),
        name="pick",
    )(order, rows)


def rows_kernel(slot, sp, cotangent, gate, weight, send, keep, rows, total):
    step = pl.program_id(0)
    scaled = (cotangent[0].astype(jnp.float32) * gate[slot : slot + 1]).astype(jnp.bfloat16)

    @pl.when(step < 2)
    def _():
        send[...] = scaled

    @pl.when(step >= 2)
    def _():
        keep[...] = scaled

    product = mm(scaled, weight[...], NT)

    @pl.when(step == 0)
    def _():
        total[...] = product

    @pl.when((step > 0) & (step < 3))
    def _():
        total[...] += product

    @pl.when(step == 3)
    def _():
        rows[...] = (total[...] + product).astype(jnp.bfloat16)


def scaled_rows(sp, slot, cotangent, gate, out_weight):
    cols = D // 4

    def place(step, sp):
        core = sp[0, 0]
        return jnp.where(step < 2, 2 * (1 - core), 2 * core - 2) + step

    def shape(cols):
        return jax.ShapeDtypeStruct((ROWS, cols), jnp.bfloat16)

    return pl.pallas_call(
        functools.partial(rows_kernel, slot),
        grid_spec=pltpu.PrefetchScalarGridSpec(
            num_scalar_prefetch=1,
            grid=(4,),
            in_specs=[
                pl.BlockSpec((1, ROWS, cols), lambda k, sp: (slot, 0, place(k, sp))),
                pl.BlockSpec((2, cols), lambda k, sp: (0, place(k, sp))),
                pl.BlockSpec((WIDTH, cols), lambda k, sp: (0, place(k, sp))),
            ],
            out_specs=[
                pl.BlockSpec((ROWS, cols), lambda k, sp: (0, jnp.minimum(k, 1))),
                pl.BlockSpec((ROWS, cols), lambda k, sp: (0, jnp.maximum(k - 2, 0))),
                pl.BlockSpec((ROWS, WIDTH), lambda k, sp: (0, 0)),
            ],
            scratch_shapes=[pltpu.VMEM((ROWS, WIDTH), jnp.float32)],
        ),
        out_shape=[shape(D // 2), shape(D // 2), shape(WIDTH)],
        cost_estimate=cost(2 * 256 * WIDTH * D, 1.3e7),
    )(sp, cotangent, gate, out_weight)


def project_kernel(sp, a0, a1, b0, b1, w_mine, w_other, gate, cotangent, mixed, gate_grad):
    mine = jnp.concatenate([a0[0], a1[0]], axis=0)
    other = jnp.concatenate([b0[0], b1[0]], axis=0)
    outputs = mm(mine, w_mine[...], NN) + mm(other, w_other[...], NN)
    for slot in range(2):
        rows = outputs[slot * ROWS : (slot + 1) * ROWS]
        mixed[slot] = (rows * gate[slot : slot + 1]).astype(jnp.bfloat16)
        gate_grad[slot : slot + 1] = jnp.sum(
            cotangent[slot].astype(jnp.float32) * rows, axis=0, keepdims=True
        )


def project(sp, mine, other, out_weight, gate, cotangent):
    cols = 1024

    def rows(index):
        return pl.BlockSpec((1, ROWS, HALF), lambda d, sp: (index, 0, 0))

    wide = pl.BlockSpec((2, ROWS, cols), lambda d, sp: (0, 0, d))
    thin = pl.BlockSpec((2, cols), lambda d, sp: (0, d))
    return pl.pallas_call(
        project_kernel,
        grid_spec=pltpu.PrefetchScalarGridSpec(
            num_scalar_prefetch=1,
            grid=(D // cols,),
            in_specs=[
                rows(0),
                rows(0),
                rows(1),
                rows(1),
                pl.BlockSpec((HALF, cols), lambda d, sp: (sp[0, 0], d)),
                pl.BlockSpec((HALF, cols), lambda d, sp: (1 - sp[0, 0], d)),
                thin,
                wide,
            ],
            out_specs=[wide, thin],
        ),
        out_shape=[
            jax.ShapeDtypeStruct((2, ROWS, D), jnp.bfloat16),
            jax.ShapeDtypeStruct((2, D), jnp.float32),
        ],
        cost_estimate=cost(2 * 512 * WIDTH * D, 1.6e7),
        name="project",
    )(sp, mine[0], mine[1], other[0], other[1], out_weight, out_weight, gate, cotangent)


def weigh_kernel(sp, own0, peer0, own1, peer1, a0, a1, b0, b1, *rest):
    outs, product = rest[:8], rest[8]
    step = pl.program_id(0)
    left = jnp.concatenate([own0[...], peer0[...], own1[...], peer1[...]], axis=0)
    mine = jnp.concatenate([a0[0], a0[1], a1[0], a1[1]], axis=0)
    other = jnp.concatenate([b0[1], b0[0], b1[1], b1[0]], axis=0)
    by_x = mm(left, mine, TN).astype(jnp.bfloat16)
    for x_step in range(4):

        @pl.when(step == x_step)
        def _():
            outs[x_step][...] = by_x

    product[...] = mm(left, other, TN)
    for y_step in range(4):
        start = pl.multiple_of((sp[1, 5] ^ y_step) * SHARE, 8)
        rows = product[pl.ds(start, SHARE), :].astype(jnp.bfloat16)
        outs[4 + y_step][sp[0, 5] ^ step] = rows


def weigh(sp, scaled, mine, other):
    rows = D // 8
    pair = pl.BlockSpec((2, ROWS, HALF), lambda d, sp: (0, 0, 0))
    wide = pl.BlockSpec((ROWS, rows), lambda d, sp: (0, sp[0, 5] ^ d))
    return pl.pallas_call(
        weigh_kernel,
        grid_spec=pltpu.PrefetchScalarGridSpec(
            num_scalar_prefetch=1,
            grid=(4,),
            in_specs=[wide] * 4 + [pair] * 4,
            out_specs=[pl.BlockSpec((rows, HALF), lambda d, sp: (0, 0))] * 4
            + [pl.BlockSpec((4, SHARE, HALF), lambda d, sp: (0, 0, 0))] * 4,
            scratch_shapes=[pltpu.VMEM((rows, HALF), jnp.float32)],
        ),
        out_shape=[jax.ShapeDtypeStruct((rows, HALF), jnp.bfloat16)] * 4
        + [jax.ShapeDtypeStruct((4, SHARE, HALF), jnp.bfloat16)] * 4,
        cost_estimate=cost(2 * 1024 * WIDTH * D // 2, 1.2e7),
        name="weigh",
    )(sp, *scaled, mine[0], mine[1], other[0], other[1])


def along_x(x, step):
    return lax.ppermute(x, "dp", [(g, g ^ (step << 3)) for g in range(32)])


def along_y(x, step):
    return lax.ppermute(x, "dp", [(g, g ^ (step << 1)) for g in range(32)])


def add_up(refs):
    total = refs[0][...].astype(jnp.float32)
    for ref in refs[1:]:
        total = total + ref[...].astype(jnp.float32)
    return total


def part_kernel(sp, *refs):
    by_x, by_y, outs, total = refs[:4], refs[4:8], refs[8:16], refs[16]
    total[...] = add_up(by_x)
    for step in range(4):
        start = pl.multiple_of((sp[1, 5] ^ step) * SHARE, 8)
        outs[step][...] = total[pl.ds(start, SHARE), :].astype(jnp.bfloat16)
    for step in range(4):
        place = sp[0, 5] ^ step
        rows = by_y[0][place].astype(jnp.float32)
        for ref in by_y[1:]:
            rows = rows + ref[place].astype(jnp.float32)
        outs[4 + step][...] = rows.astype(jnp.bfloat16)


def sum_parts(sp, by_x, by_y):
    cols = HALF // 2
    share = pl.BlockSpec((SHARE, cols), lambda i, sp: (0, i))
    return pl.pallas_call(
        part_kernel,
        grid_spec=pltpu.PrefetchScalarGridSpec(
            num_scalar_prefetch=1,
            grid=(2,),
            in_specs=[pl.BlockSpec((4 * SHARE, cols), lambda i, sp: (0, i))] * 4
            + [pl.BlockSpec((4, SHARE, cols), lambda i, sp: (0, 0, i))] * 4,
            out_specs=[share] * 8,
            scratch_shapes=[pltpu.VMEM((4 * SHARE, cols), jnp.float32)],
        ),
        out_shape=[jax.ShapeDtypeStruct((SHARE, HALF), jnp.bfloat16)] * 8,
        cost_estimate=cost(5e6, 6e6),
        name="sum_parts",
    )(sp, *by_x, *by_y)


def final_moves(step):
    moves = []
    for xy in range(16):
        for z_low in range(2):
            for z_high in range(2):
                for core in range(2):
                    source = 4 * (2 * xy + z_low) + 2 * z_high + core
                    target = 4 * (16 * core + xy) + ((2 * z_low + z_high) ^ step)
                    moves.append((source, target))
    return moves


def sum_kernel(sp, *refs):
    low, high, outs, total = refs[:4], refs[4:8], refs[8:12], refs[12]
    first = sp[0, 0] == 0
    mine = add_up(low)
    other = add_up(high)
    total[:, :HALF] = jnp.where(first, mine, other)
    total[:, HALF:] = jnp.where(first, other, mine)
    count = SHARE // 4
    for step, out in enumerate(outs):
        start = pl.multiple_of((sp[1, 0] ^ step) * count, 8)
        out[...] = total[pl.ds(start, count), :].astype(jnp.bfloat16)


def sum_weights(sp, low, high):
    def whole(rows, cols):
        return pl.BlockSpec((rows, cols), lambda i, sp: (0, 0))

    return pl.pallas_call(
        sum_kernel,
        grid_spec=pltpu.PrefetchScalarGridSpec(
            num_scalar_prefetch=1,
            grid=(1,),
            in_specs=[whole(SHARE, HALF)] * 8,
            out_specs=[whole(SHARE // 4, WIDTH)] * 4,
            scratch_shapes=[pltpu.VMEM((SHARE, WIDTH), jnp.float32)],
        ),
        out_shape=[jax.ShapeDtypeStruct((SHARE // 4, WIDTH), jnp.bfloat16)] * 4,
        cost_estimate=cost(1e6, 2e6),
        name="sum_weights",
    )(sp, *low, *high)


def finish_weights(quarters):
    pieces = [
        lax.ppermute(quarter, ("dp", "seq"), final_moves(step)).astype(jnp.float32)
        for step, quarter in enumerate(quarters)
    ]
    return (pieces[0] + pieces[1] + pieces[2] + pieces[3]).T


def after(value, *others):
    return lax.optimization_barrier((value, *others))[0]


def spread_out(rows):
    groups = lax.axis_size("dp")
    portions = rows.reshape(groups, -1, rows.shape[-1])
    return lax.all_to_all(portions, "dp", split_axis=0, concat_axis=0, tiled=True)


def land(arranged, shape):
    landed = lax.all_to_all(arranged, "dp", split_axis=0, concat_axis=0, tiled=True)
    return landed.reshape(shape)


def body(qkv, gate, cotangent, out_weight, clip_lengths, text_lengths, plan):
    groups = lax.axis_size("dp")
    group_index = lax.axis_index("dp")
    seq_index = lax.axis_index("seq")
    core = seq_index & 1
    z_place = 2 * (group_index & 1) + (seq_index >> 1)
    ordinal = jnp.arange(groups, dtype=jnp.int32)
    inverse = jnp.sum(jnp.where(plan[None, :] == ordinal[:, None], ordinal[None, :], 0), axis=1)

    quarters = seq_index ^ jnp.arange(4, dtype=jnp.int32)
    text = lax.dynamic_slice_in_dim(text_lengths, 2 * group_index, 2)[:, None]
    video = lax.dynamic_slice_in_dim(clip_lengths, 2 * group_index, 2)[:, None]
    limits = jnp.where(quarters[None] == 0, text, video - (quarters[None] - 1) * ROWS)
    place = jnp.stack([core, z_place]).astype(jnp.int32)[:, None]
    plane = jnp.stack([group_index >> 3, (group_index >> 1) & 3]).astype(jnp.int32)[:, None]
    sp = jnp.concatenate([place, limits.astype(jnp.int32), plane], axis=1)

    def to_core(rows):
        return swap(rows[None], 1)

    received = [None, None]
    d_own, d_peer = [None, None], [None, None]
    att, lse = [None, None], [None, None]

    cp = core.astype(jnp.int32).reshape(1, 1)
    s1, s2, s3 = prep(cp, qkv, 1)
    near_keys = (swap(s1, 1), swap(s3, 3))
    received[1] = (near_keys[0], swap(s2, 2), near_keys[1])
    send_1, keep_1, away = scaled_rows(after(cp, s2), 1, cotangent, gate, out_weight)
    d_spread = spread_out(away)
    send_0, keep_0, near = scaled_rows(after(cp, away), 0, cotangent, gate, out_weight)
    d_own[0], d_peer[0] = near[None], to_core(near)
    scaled = (keep_0, swap(send_0, 1), keep_1, swap(send_1, 1))
    d_picked = pick(d_spread, after(plan, near, sp))
    landed = land(d_picked, (ROWS, WIDTH))
    s1, s2, s3 = prep(after(cp, d_picked), qkv, 0)
    received[0] = (swap(s1, 1), swap(s2, 2), swap(s3, 3))
    sp = after(sp, s2)
    att[1], lse[1] = attend(sp, 1, qkv, received[1])
    d_own[1], d_peer[1] = landed[None], to_core(landed)
    att_spread = spread_out(after(att[1], landed).reshape(2 * ROWS, HALF))

    def back(sp, slot):
        return attend_back(
            sp, slot, qkv, received[slot], att[slot], lse[slot], d_own[slot], d_peer[slot]
        )

    own_1, r1, r2, r3 = back(sp, 1)
    pieces_1 = (swap(r1, 1), swap(r3, 3))
    pieces_1 = (pieces_1[0], swap(r2, 2), pieces_1[1])
    att[0], lse[0] = attend(after(sp, r2), 0, qkv, received[0])
    att_other = [swap(att[0], 1)]
    picked = pick(att_spread, after(inverse, lse[0]))
    moved = land(picked, (2, ROWS, HALF))
    own_0, *sent_0 = back(after(sp, picked), 0)
    pieces_0 = [swap(rows, 1 + i) for i, rows in enumerate(sent_0)]
    balanced = [att[0], moved]
    att_other.append(swap(moved, 1))
    *partial, = weigh(after(sp, sent_0[1]), scaled, balanced, att_other)
    by_x, by_y = partial[:4], partial[4:]
    for step in (2, 1, 3):
        by_x[step] = along_x(by_x[step], step)
        by_y[step] = along_y(by_y[step], step)
    mixed, gate_part = project(
        after(sp, partial[0]), balanced, att_other, out_weight, gate, cotangent
    )
    gate_grad = gate_part + swap(gate_part, 1) + swap(gate_part, 2) + swap(gate_part, 3)
    grads = join(after(sp, gate_part), 1, own_1, *pieces_1, None)
    parts = list(sum_parts(after(sp, grads), by_x, by_y))
    low = parts[:1] + [along_y(parts[step], step) for step in (1, 2, 3)]
    high = parts[4:5] + [along_x(parts[4 + step], step) for step in (1, 2, 3)]
    grads = join(after(sp, parts[0]), 0, own_0, *pieces_0, grads)
    quarters = sum_weights(after(sp, grads), low, high)
    weight_grad = finish_weights(quarters)
    return (mixed, gate_grad, weight_grad, grads)


def solution(mesh):
    in_specs = (P("dp", "seq", None), P("dp", None), P("dp", "seq", None), P(), P(), P(), P())
    out_specs = (P("dp", "seq", None), P("dp", None), P(None, ("dp", "seq")), P("dp", "seq", None))
    return jax.shard_map(body, mesh=mesh, in_specs=in_specs, out_specs=out_specs, check_vma=False)
```

```python
import functools

import jax
import jax.numpy as jnp
from jax import lax
from jax.experimental import pallas as pl
from jax.experimental.pallas import tpu as pltpu
from jax.sharding import PartitionSpec as P


HD = 128
ROWS = 256
HEADS_HALF = 6
HALF = HEADS_HALF * HD
WIDTH = 2 * HALF
TOGETHER = 2
TOGETHER_BACK = 2
SHARE = 96
D = 3072
NEGATIVE = -1e30
LOG2E = 1.4426950408889634
SCALE = HD**-0.5

NT = (((1,), (1,)), ((), ()))
NN = (((1,), (0,)), ((), ()))
TN = (((0,), (0,)), ((), ()))


def mm(a, b, dims):
    return lax.dot_general(a, b, dims, preferred_element_type=jnp.float32)


def cost(flops, nbytes, transcendentals=0):
    return pl.CostEstimate(
        flops=int(flops), bytes_accessed=int(nbytes), transcendentals=int(transcendentals)
    )


def swap(x, step):
    return lax.ppermute(x, "seq", [(i, i ^ step) for i in range(4)])


def prep_kernel(sp, qo, ko, vo, kc, vc, s1, s2, s3):
    s1[0] = qo[0]
    s1[1] = ko[0]
    s1[2] = vo[0]
    s2[0] = kc[0]
    s2[1] = vc[0]
    s3[0] = ko[0]
    s3[1] = vo[0]


def prep(sp, qkv, slot):
    rows = ROWS // 2

    def half(member, other):
        def index(r, sp):
            core = sp[0, 0]
            return (slot, r, 2 * member + (1 - core if other else core))

        return pl.BlockSpec((1, rows, HALF), index)

    def out(count):
        return pl.BlockSpec((count, rows, HALF), lambda r, sp: (0, r, 0))

    def shape(count):
        return jax.ShapeDtypeStruct((count, ROWS, HALF), jnp.bfloat16)

    return pl.pallas_call(
        prep_kernel,
        grid_spec=pltpu.PrefetchScalarGridSpec(
            num_scalar_prefetch=1,
            grid=(2,),
            in_specs=[half(0, True), half(1, True), half(2, True), half(1, False), half(2, False)],
            out_specs=[out(3), out(2), out(2)],
        ),
        out_shape=[shape(3), shape(2), shape(2)],
        cost_estimate=cost(1e6, 5e6),
    )(sp, qkv, qkv, qkv, qkv, qkv)


def live_limit(sp, slot, block, shape, axis):
    return lax.broadcasted_iota(jnp.int32, shape, axis) < sp[slot, 1 + block]


def key_bias(sp, slot, axis):
    shape = (ROWS, 1) if axis == 0 else (1, ROWS)
    parts = [
        jnp.where(live_limit(sp, slot, block, shape, axis), 0.0, NEGATIVE) for block in range(4)
    ]
    return jnp.concatenate(parts, axis=axis)


def fwd_kernel(slot, sp, q0, k0, v0, q1, k1, v1, k2, v2, k3, v3, att, lse):
    bias = key_bias(sp, slot, 1)
    work = []
    for head in range(TOGETHER):
        cols = slice(head * HD, (head + 1) * HD)
        keys = jnp.concatenate([k[0, :, cols] for k in (k0, k1, k2, k3)], axis=0)
        values = jnp.concatenate([v[0, :, cols] for v in (v0, v1, v2, v3)], axis=0)
        for block, q in enumerate((q0, q1)):
            work.append((head, cols, block, mm(q[0, :, cols], keys, NT), values))
    for head, cols, block, products, values in work:
        scores = products * (SCALE * LOG2E) + bias
        peak = jnp.max(scores, axis=1, keepdims=True)
        powers = jnp.exp2(scores - peak)
        total = jnp.sum(powers, axis=1, keepdims=True)
        live = live_limit(sp, slot, block, (ROWS, 1), 0)
        inverse = jnp.where(live, 1.0 / total, 0.0)
        mixed = mm(powers.astype(jnp.bfloat16), values, NN) * inverse
        att[block, :, cols] = mixed.astype(jnp.bfloat16)
        level = jnp.where(live, peak + jnp.log2(total), -NEGATIVE)
        lse[head, :, block * ROWS : (block + 1) * ROWS] = jnp.broadcast_to(level, (ROWS, HD)).T[:8]


def bwd_kernel(
    slot, sp, q0, k0, v0, q1, k1, v1, k2, v2, k3, v3, att, lse, do0, do1, own, r1, r2, r3
):
    bias = key_bias(sp, slot, 0)
    low = jnp.bfloat16
    for head in range(TOGETHER_BACK):
        cols = slice(head * HD, (head + 1) * HD)
        keys = jnp.concatenate([k[0, :, cols] for k in (k0, k1, k2, k3)], axis=0)
        values = jnp.concatenate([v[0, :, cols] for v in (v0, v1, v2, v3)], axis=0)
        grad_k = None
        grad_v = None
        for block, (q, do) in enumerate(((q0, do0), (q1, do1))):
            q_rows = q[0, :, cols]
            d_rows = do[0, :, cols]
            scores = mm(keys, q_rows, NT) * (SCALE * LOG2E) + bias
            level = lse[head, 0:1, block * ROWS : (block + 1) * ROWS]
            probs = jnp.exp2(scores - level)
            product = d_rows.astype(jnp.float32) * att[block, :, cols].astype(jnp.float32)
            dots = jnp.sum(product.T, axis=0, keepdims=True)
            d_probs = mm(values, d_rows, NT)
            d_scores = (probs * (d_probs - dots)).astype(low)
            v_part = mm(probs.astype(low), d_rows, NN)
            k_part = mm(d_scores, q_rows, NN)
            grad_k = k_part if block == 0 else grad_k + k_part
            grad_v = v_part if block == 0 else grad_v + v_part
            grad_q = (mm(keys, d_scores, TN) * SCALE).T
            if block == 0:
                own[0, :, cols] = grad_q
            else:
                r1[0, :, cols] = grad_q.astype(low)
        grad_k = grad_k * SCALE
        own[1, :, cols] = grad_k[:ROWS]
        own[2, :, cols] = grad_v[:ROWS]
        r1[1, :, cols] = grad_k[ROWS : 2 * ROWS].astype(low)
        r1[2, :, cols] = grad_v[ROWS : 2 * ROWS].astype(low)
        r2[0, :, cols] = grad_k[2 * ROWS : 3 * ROWS].astype(low)
        r2[1, :, cols] = grad_v[2 * ROWS : 3 * ROWS].astype(low)
        r3[0, :, cols] = grad_k[3 * ROWS :].astype(low)
        r3[1, :, cols] = grad_v[3 * ROWS :].astype(low)


def head_block(lead, index=0, heads=1):
    return pl.BlockSpec((lead, ROWS, heads * HD), lambda h, sp: (index, 0, h))


def section_specs(slot, heads=1):
    def own(member):
        return pl.BlockSpec(
            (1, ROWS, heads * HD),
            lambda h, sp: (slot, 0, (12 * member + HEADS_HALF * sp[0, 0]) // heads + h),
        )

    return [own(0), own(1), own(2)] + [head_block(1, m, heads) for m in (0, 1, 2, 0, 1, 0, 1)]


def sections(qkv, x1, x2, x3):
    return (qkv, qkv, qkv, x1, x1, x1, x2, x2, x3, x3)


PAIRS = HEADS_HALF * 512 * 1024


def attend(sp, slot, qkv, received):
    return pl.pallas_call(
        functools.partial(fwd_kernel, slot),
        grid_spec=pltpu.PrefetchScalarGridSpec(
            num_scalar_prefetch=1,
            grid=(HEADS_HALF // TOGETHER,),
            in_specs=section_specs(slot, TOGETHER),
            out_specs=[
                head_block(2, 0, TOGETHER),
                pl.BlockSpec((TOGETHER, 8, 2 * ROWS), lambda h, sp: (h, 0, 0)),
            ],
        ),
        out_shape=[
            jax.ShapeDtypeStruct((2, ROWS, HALF), jnp.bfloat16),
            jax.ShapeDtypeStruct((HEADS_HALF, 8, 2 * ROWS), jnp.float32),
        ],
        cost_estimate=cost(4 * PAIRS * HD, 5e6, PAIRS),
    )(sp, *sections(qkv, *received))


def attend_back(sp, slot, qkv, received, att, lse, d_own, d_peer):
    heads = TOGETHER_BACK
    d_own_spec = pl.BlockSpec(
        (1, ROWS, heads * HD), lambda h, sp: (0, 0, HEADS_HALF // heads * sp[0, 0] + h)
    )

    def shape(count, kind):
        return jax.ShapeDtypeStruct((count, ROWS, HALF), kind)

    def piece(count):
        return head_block(count, 0, heads)

    return pl.pallas_call(
        functools.partial(bwd_kernel, slot),
        grid_spec=pltpu.PrefetchScalarGridSpec(
            num_scalar_prefetch=1,
            grid=(HEADS_HALF // heads,),
            in_specs=section_specs(slot, heads)
            + [
                piece(2),
                pl.BlockSpec((heads, 8, 2 * ROWS), lambda h, sp: (h, 0, 0)),
                d_own_spec,
                d_own_spec,
            ],
            out_specs=[piece(3), piece(3), piece(2), piece(2)],
        ),
        out_shape=[
            shape(3, jnp.float32),
            shape(3, jnp.bfloat16),
            shape(2, jnp.bfloat16),
            shape(2, jnp.bfloat16),
        ],
        cost_estimate=cost(10 * PAIRS * HD, 1e7, PAIRS),
    )(sp, *sections(qkv, *received), att, lse, d_own, d_peer)


def join_kernel(sp, own, p1, p2, p3, *rest):
    out = rest[-1]
    core = sp[0, 0]
    member = pl.program_id(0)
    crossing = jnp.where(member > 0, 1.0, 0.0)
    mine = own[0] + crossing * p2[0].astype(jnp.float32)
    other = p1[0].astype(jnp.float32) + crossing * p3[0].astype(jnp.float32)
    first = core == 0
    out[0, :, :HALF] = jnp.where(first, mine, other).astype(jnp.bfloat16)
    out[0, :, HALF:] = jnp.where(first, other, mine).astype(jnp.bfloat16)


def join(sp, slot, own, p1, p2, p3, base):
    def piece(shift):
        return pl.BlockSpec((1, ROWS, HALF), lambda m, sp: (jnp.maximum(m - shift, 0), 0, 0))

    in_specs = [piece(0), piece(0), piece(1), piece(1)]
    args = [own, p1, p2, p3]
    aliases = {}
    if base is not None:
        in_specs.append(pl.BlockSpec(memory_space=pl.ANY))
        args.append(base)
        aliases = {5: 0}
    return pl.pallas_call(
        join_kernel,
        grid_spec=pltpu.PrefetchScalarGridSpec(
            num_scalar_prefetch=1,
            grid=(3,),
            in_specs=in_specs,
            out_specs=pl.BlockSpec((1, ROWS, WIDTH), lambda m, sp: (slot, 0, m)),
        ),
        out_shape=jax.ShapeDtypeStruct((2, ROWS, 3 * WIDTH), jnp.bfloat16),
        input_output_aliases=aliases,
        cost_estimate=cost(1e6, 1e7),
    )(sp, *args)


def pick_kernel(order, rows, out):
    def step(slot, carry):
        out[slot] = rows[order[slot]]
        return carry

    lax.fori_loop(0, rows.shape[0], step, 0)


def pick(rows, order):
    whole = pl.BlockSpec(rows.shape, lambda i, order: (0, 0, 0))
    return pl.pallas_call(
        pick_kernel,
        grid_spec=pltpu.PrefetchScalarGridSpec(
            num_scalar_prefetch=1, grid=(1,), in_specs=[whole], out_specs=whole
        ),
        out_shape=jax.ShapeDtypeStruct(rows.shape, rows.dtype),
        cost_estimate=cost(1e6, 2 * rows.size * 2),
    )(order, rows)


def rows_kernel(slot, sp, cotangent, gate, weight, send, keep, rows, total):
    step = pl.program_id(0)
    scaled = (cotangent[0].astype(jnp.float32) * gate[slot : slot + 1]).astype(jnp.bfloat16)

    @pl.when(step < 2)
    def _():
        send[...] = scaled

    @pl.when(step >= 2)
    def _():
        keep[...] = scaled

    product = mm(scaled, weight[...], NT)

    @pl.when(step == 0)
    def _():
        total[...] = product

    @pl.when((step > 0) & (step < 3))
    def _():
        total[...] += product

    @pl.when(step == 3)
    def _():
        rows[...] = (total[...] + product).astype(jnp.bfloat16)


def scaled_rows(sp, slot, cotangent, gate, out_weight):
    cols = D // 4

    def place(step, sp):
        core = sp[0, 0]
        return jnp.where(step < 2, 2 * (1 - core), 2 * core - 2) + step

    def shape(cols):
        return jax.ShapeDtypeStruct((ROWS, cols), jnp.bfloat16)

    return pl.pallas_call(
        functools.partial(rows_kernel, slot),
        grid_spec=pltpu.PrefetchScalarGridSpec(
            num_scalar_prefetch=1,
            grid=(4,),
            in_specs=[
                pl.BlockSpec((1, ROWS, cols), lambda k, sp: (slot, 0, place(k, sp))),
                pl.BlockSpec((2, cols), lambda k, sp: (0, place(k, sp))),
                pl.BlockSpec((WIDTH, cols), lambda k, sp: (0, place(k, sp))),
            ],
            out_specs=[
                pl.BlockSpec((ROWS, cols), lambda k, sp: (0, jnp.minimum(k, 1))),
                pl.BlockSpec((ROWS, cols), lambda k, sp: (0, jnp.maximum(k - 2, 0))),
                pl.BlockSpec((ROWS, WIDTH), lambda k, sp: (0, 0)),
            ],
            scratch_shapes=[pltpu.VMEM((ROWS, WIDTH), jnp.float32)],
        ),
        out_shape=[shape(D // 2), shape(D // 2), shape(WIDTH)],
        cost_estimate=cost(2 * 256 * WIDTH * D, 1.3e7),
    )(sp, cotangent, gate, out_weight)


def project_kernel(sp, a0, a1, b0, b1, w_mine, w_other, gate, cotangent, mixed, gate_grad):
    mine = jnp.concatenate([a0[0], a1[0]], axis=0)
    other = jnp.concatenate([b0[0], b1[0]], axis=0)
    outputs = mm(mine, w_mine[...], NN) + mm(other, w_other[...], NN)
    for slot in range(2):
        rows = outputs[slot * ROWS : (slot + 1) * ROWS]
        mixed[slot] = (rows * gate[slot : slot + 1]).astype(jnp.bfloat16)
        gate_grad[slot : slot + 1] = jnp.sum(
            cotangent[slot].astype(jnp.float32) * rows, axis=0, keepdims=True
        )


def project(sp, mine, other, out_weight, gate, cotangent):
    cols = 1024

    def rows(index):
        return pl.BlockSpec((1, ROWS, HALF), lambda d, sp: (index, 0, 0))

    wide = pl.BlockSpec((2, ROWS, cols), lambda d, sp: (0, 0, d))
    thin = pl.BlockSpec((2, cols), lambda d, sp: (0, d))
    return pl.pallas_call(
        project_kernel,
        grid_spec=pltpu.PrefetchScalarGridSpec(
            num_scalar_prefetch=1,
            grid=(D // cols,),
            in_specs=[
                rows(0),
                rows(0),
                rows(1),
                rows(1),
                pl.BlockSpec((HALF, cols), lambda d, sp: (sp[0, 0], d)),
                pl.BlockSpec((HALF, cols), lambda d, sp: (1 - sp[0, 0], d)),
                thin,
                wide,
            ],
            out_specs=[wide, thin],
        ),
        out_shape=[
            jax.ShapeDtypeStruct((2, ROWS, D), jnp.bfloat16),
            jax.ShapeDtypeStruct((2, D), jnp.float32),
        ],
        cost_estimate=cost(2 * 512 * WIDTH * D, 1.6e7),
    )(sp, mine[0], mine[1], other[0], other[1], out_weight, out_weight, gate, cotangent)


def weigh_kernel(sp, own0, peer0, own1, peer1, a0, a1, b0, b1, *rest):
    outs, product = rest[:8], rest[8]
    step = pl.program_id(0)
    left = jnp.concatenate([own0[...], peer0[...], own1[...], peer1[...]], axis=0)
    mine = jnp.concatenate([a0[0], a0[1], a1[0], a1[1]], axis=0)
    other = jnp.concatenate([b0[1], b0[0], b1[1], b1[0]], axis=0)
    by_x = mm(left, mine, TN).astype(jnp.bfloat16)
    for x_step in range(4):

        @pl.when(step == x_step)
        def _():
            outs[x_step][...] = by_x

    product[...] = mm(left, other, TN)
    for y_step in range(4):
        start = pl.multiple_of((sp[1, 5] ^ y_step) * SHARE, 8)
        rows = product[pl.ds(start, SHARE), :].astype(jnp.bfloat16)
        outs[4 + y_step][sp[0, 5] ^ step] = rows


def weigh(sp, scaled, mine, other):
    rows = D // 8
    pair = pl.BlockSpec((2, ROWS, HALF), lambda d, sp: (0, 0, 0))
    wide = pl.BlockSpec((ROWS, rows), lambda d, sp: (0, sp[0, 5] ^ d))
    return pl.pallas_call(
        weigh_kernel,
        grid_spec=pltpu.PrefetchScalarGridSpec(
            num_scalar_prefetch=1,
            grid=(4,),
            in_specs=[wide] * 4 + [pair] * 4,
            out_specs=[pl.BlockSpec((rows, HALF), lambda d, sp: (0, 0))] * 4
            + [pl.BlockSpec((4, SHARE, HALF), lambda d, sp: (0, 0, 0))] * 4,
            scratch_shapes=[pltpu.VMEM((rows, HALF), jnp.float32)],
        ),
        out_shape=[jax.ShapeDtypeStruct((rows, HALF), jnp.bfloat16)] * 4
        + [jax.ShapeDtypeStruct((4, SHARE, HALF), jnp.bfloat16)] * 4,
        cost_estimate=cost(2 * 1024 * WIDTH * D // 2, 1.2e7),
    )(sp, *scaled, mine[0], mine[1], other[0], other[1])


def along_x(x, step):
    return lax.ppermute(x, "dp", [(g, g ^ (step << 3)) for g in range(32)])


def along_y(x, step):
    return lax.ppermute(x, "dp", [(g, g ^ (step << 1)) for g in range(32)])


def add_up(refs):
    total = refs[0][...].astype(jnp.float32)
    for ref in refs[1:]:
        total = total + ref[...].astype(jnp.float32)
    return total


def part_kernel(sp, *refs):
    by_x, by_y, outs, total = refs[:4], refs[4:8], refs[8:16], refs[16]
    total[...] = add_up(by_x)
    for step in range(4):
        start = pl.multiple_of((sp[1, 5] ^ step) * SHARE, 8)
        outs[step][...] = total[pl.ds(start, SHARE), :].astype(jnp.bfloat16)
    for step in range(4):
        place = sp[0, 5] ^ step
        rows = by_y[0][place].astype(jnp.float32)
        for ref in by_y[1:]:
            rows = rows + ref[place].astype(jnp.float32)
        outs[4 + step][...] = rows.astype(jnp.bfloat16)


def sum_parts(sp, by_x, by_y):
    cols = HALF // 2
    share = pl.BlockSpec((SHARE, cols), lambda i, sp: (0, i))
    return pl.pallas_call(
        part_kernel,
        grid_spec=pltpu.PrefetchScalarGridSpec(
            num_scalar_prefetch=1,
            grid=(2,),
            in_specs=[pl.BlockSpec((4 * SHARE, cols), lambda i, sp: (0, i))] * 4
            + [pl.BlockSpec((4, SHARE, cols), lambda i, sp: (0, 0, i))] * 4,
            out_specs=[share] * 8,
            scratch_shapes=[pltpu.VMEM((4 * SHARE, cols), jnp.float32)],
        ),
        out_shape=[jax.ShapeDtypeStruct((SHARE, HALF), jnp.bfloat16)] * 8,
        cost_estimate=cost(5e6, 6e6),
    )(sp, *by_x, *by_y)


def final_moves(step):
    moves = []
    for xy in range(16):
        for z_low in range(2):
            for z_high in range(2):
                for core in range(2):
                    source = 4 * (2 * xy + z_low) + 2 * z_high + core
                    target = 4 * (16 * core + xy) + ((2 * z_low + z_high) ^ step)
                    moves.append((source, target))
    return moves


def sum_kernel(sp, *refs):
    low, high, outs, total = refs[:4], refs[4:8], refs[8:12], refs[12]
    first = sp[0, 0] == 0
    mine = add_up(low)
    other = add_up(high)
    total[:, :HALF] = jnp.where(first, mine, other)
    total[:, HALF:] = jnp.where(first, other, mine)
    count = SHARE // 4
    for step, out in enumerate(outs):
        start = pl.multiple_of((sp[1, 0] ^ step) * count, 8)
        out[...] = total[pl.ds(start, count), :].astype(jnp.bfloat16)


def sum_weights(sp, low, high):
    def whole(rows, cols):
        return pl.BlockSpec((rows, cols), lambda i, sp: (0, 0))

    return pl.pallas_call(
        sum_kernel,
        grid_spec=pltpu.PrefetchScalarGridSpec(
            num_scalar_prefetch=1,
            grid=(1,),
            in_specs=[whole(SHARE, HALF)] * 8,
            out_specs=[whole(SHARE // 4, WIDTH)] * 4,
            scratch_shapes=[pltpu.VMEM((SHARE, WIDTH), jnp.float32)],
        ),
        out_shape=[jax.ShapeDtypeStruct((SHARE // 4, WIDTH), jnp.bfloat16)] * 4,
        cost_estimate=cost(1e6, 2e6),
    )(sp, *low, *high)


def finish_weights(quarters):
    pieces = [
        lax.ppermute(quarter, ("dp", "seq"), final_moves(step)).astype(jnp.float32)
        for step, quarter in enumerate(quarters)
    ]
    return (pieces[0] + pieces[1] + pieces[2] + pieces[3]).T


def after(value, *others):
    return lax.optimization_barrier((value, *others))[0]


def spread_out(rows):
    groups = lax.axis_size("dp")
    portions = rows.reshape(groups, -1, rows.shape[-1])
    return lax.all_to_all(portions, "dp", split_axis=0, concat_axis=0, tiled=True)


def land(arranged, shape):
    landed = lax.all_to_all(arranged, "dp", split_axis=0, concat_axis=0, tiled=True)
    return landed.reshape(shape)


def body(qkv, gate, cotangent, out_weight, clip_lengths, text_lengths, plan):
    groups = lax.axis_size("dp")
    group_index = lax.axis_index("dp")
    seq_index = lax.axis_index("seq")
    core = seq_index & 1
    z_place = 2 * (group_index & 1) + (seq_index >> 1)
    ordinal = jnp.arange(groups, dtype=jnp.int32)
    inverse = jnp.sum(jnp.where(plan[None, :] == ordinal[:, None], ordinal[None, :], 0), axis=1)

    quarters = seq_index ^ jnp.arange(4, dtype=jnp.int32)
    text = lax.dynamic_slice_in_dim(text_lengths, 2 * group_index, 2)[:, None]
    video = lax.dynamic_slice_in_dim(clip_lengths, 2 * group_index, 2)[:, None]
    limits = jnp.where(quarters[None] == 0, text, video - (quarters[None] - 1) * ROWS)
    place = jnp.stack([core, z_place]).astype(jnp.int32)[:, None]
    plane = jnp.stack([group_index >> 3, (group_index >> 1) & 3]).astype(jnp.int32)[:, None]
    sp = jnp.concatenate([place, limits.astype(jnp.int32), plane], axis=1)

    def to_core(rows):
        return swap(rows[None], 1)

    received = [None, None]
    d_own, d_peer = [None, None], [None, None]
    att, lse = [None, None], [None, None]

    cp = core.astype(jnp.int32).reshape(1, 1)
    s1, s2, s3 = prep(cp, qkv, 1)
    near_keys = (swap(s1, 1), swap(s3, 3))
    received[1] = (near_keys[0], swap(s2, 2), near_keys[1])
    send_1, keep_1, away = scaled_rows(after(cp, s2), 1, cotangent, gate, out_weight)
    d_spread = spread_out(away)
    send_0, keep_0, near = scaled_rows(after(cp, away), 0, cotangent, gate, out_weight)
    d_own[0], d_peer[0] = near[None], to_core(near)
    scaled = (keep_0, swap(send_0, 1), keep_1, swap(send_1, 1))
    d_picked = pick(d_spread, after(plan, near, sp))
    landed = land(d_picked, (ROWS, WIDTH))
    s1, s2, s3 = prep(after(cp, d_picked), qkv, 0)
    near_keys = (swap(s1, 1), swap(s3, 3))
    received[0] = (near_keys[0], swap(s2, 2), near_keys[1])
    sp = after(sp, s2)
    att[1], lse[1] = attend(sp, 1, qkv, received[1])
    d_own[1], d_peer[1] = landed[None], to_core(landed)
    att_spread = spread_out(after(att[1], landed).reshape(2 * ROWS, HALF))

    def back(sp, slot):
        return attend_back(
            sp, slot, qkv, received[slot], att[slot], lse[slot], d_own[slot], d_peer[slot]
        )

    own_1, r1, r2, r3 = back(sp, 1)
    picked = pick(att_spread, after(inverse, r2))
    moved = land(picked, (2, ROWS, HALF))
    pieces_1 = (swap(r1, 1), swap(r2, 2), swap(r3, 3))
    att[0], lse[0] = attend(after(sp, picked), 0, qkv, received[0])
    att_other = [swap(att[0], 1)]
    own_0, *sent_0 = back(after(sp, lse[0]), 0)
    pieces_0 = [swap(rows, 1 + i) for i, rows in enumerate(sent_0)]
    balanced = [att[0], moved]
    att_other.append(swap(moved, 1))
    *partial, = weigh(after(sp, sent_0[1]), scaled, balanced, att_other)
    by_x, by_y = partial[:4], partial[4:]
    for step in (2, 1, 3):
        by_x[step] = along_x(by_x[step], step)
        by_y[step] = along_y(by_y[step], step)
    mixed, gate_part = project(
        after(sp, partial[0]), balanced, att_other, out_weight, gate, cotangent
    )
    gate_grad = gate_part + swap(gate_part, 1) + swap(gate_part, 2) + swap(gate_part, 3)
    grads = join(after(sp, gate_part), 1, own_1, *pieces_1, None)
    parts = list(sum_parts(after(sp, grads), by_x, by_y))
    low = parts[:1] + [along_y(parts[step], step) for step in (1, 2, 3)]
    high = parts[4:5] + [along_x(parts[4 + step], step) for step in (1, 2, 3)]
    grads = join(after(sp, parts[0]), 0, own_0, *pieces_0, grads)
    quarters = sum_weights(after(sp, grads), low, high)
    weight_grad = finish_weights(quarters)
    return (mixed, gate_grad, weight_grad, grads)


def solution(mesh):
    in_specs = (P("dp", "seq", None), P("dp", None), P("dp", "seq", None), P(), P(), P(), P())
    out_specs = (P("dp", "seq", None), P("dp", None), P(None, ("dp", "seq")), P("dp", "seq", None))
    return jax.shard_map(body, mesh=mesh, in_specs=in_specs, out_specs=out_specs, check_vma=False)
```

```python
import functools

import jax
import jax.numpy as jnp
from jax import lax
from jax.experimental import pallas as pl
from jax.experimental.pallas import tpu as pltpu
from jax.sharding import PartitionSpec as P


HD = 128
ROWS = 256
HEADS_HALF = 6
HALF = HEADS_HALF * HD
WIDTH = 2 * HALF
TOGETHER = 2
TOGETHER_BACK = 2
SHARE = 96
D = 3072
NEGATIVE = -1e30
LOG2E = 1.4426950408889634
SCALE = HD**-0.5

NT = (((1,), (1,)), ((), ()))
NN = (((1,), (0,)), ((), ()))
TN = (((0,), (0,)), ((), ()))


def mm(a, b, dims):
    return lax.dot_general(a, b, dims, preferred_element_type=jnp.float32)


def cost(flops, nbytes, transcendentals=0):
    return pl.CostEstimate(
        flops=int(flops), bytes_accessed=int(nbytes), transcendentals=int(transcendentals)
    )


def swap(x, step):
    return lax.ppermute(x, "seq", [(i, i ^ step) for i in range(4)])


def prep_kernel(sp, qo, ko, vo, kc, vc, s1, s2, s3):
    s1[0] = qo[0]
    s1[1] = ko[0]
    s1[2] = vo[0]
    s2[0] = kc[0]
    s2[1] = vc[0]
    s3[0] = ko[0]
    s3[1] = vo[0]


def prep(sp, qkv, slot):
    rows = ROWS // 2

    def half(member, other):
        def index(r, sp):
            core = sp[0, 0]
            return (slot, r, 2 * member + (1 - core if other else core))

        return pl.BlockSpec((1, rows, HALF), index)

    def out(count):
        return pl.BlockSpec((count, rows, HALF), lambda r, sp: (0, r, 0))

    def shape(count):
        return jax.ShapeDtypeStruct((count, ROWS, HALF), jnp.bfloat16)

    return pl.pallas_call(
        prep_kernel,
        grid_spec=pltpu.PrefetchScalarGridSpec(
            num_scalar_prefetch=1,
            grid=(2,),
            in_specs=[half(0, True), half(1, True), half(2, True), half(1, False), half(2, False)],
            out_specs=[out(3), out(2), out(2)],
        ),
        out_shape=[shape(3), shape(2), shape(2)],
        cost_estimate=cost(1e6, 5e6),
    )(sp, qkv, qkv, qkv, qkv, qkv)


def live_limit(sp, slot, block, shape, axis):
    return lax.broadcasted_iota(jnp.int32, shape, axis) < sp[slot, 1 + block]


def key_bias(sp, slot, axis):
    shape = (ROWS, 1) if axis == 0 else (1, ROWS)
    parts = [
        jnp.where(live_limit(sp, slot, block, shape, axis), 0.0, NEGATIVE) for block in range(4)
    ]
    return jnp.concatenate(parts, axis=axis)


def fwd_kernel(slot, sp, q0, k0, v0, q1, k1, v1, k2, v2, k3, v3, att, lse):
    bias = key_bias(sp, slot, 1)
    work = []
    for head in range(TOGETHER):
        cols = slice(head * HD, (head + 1) * HD)
        keys = jnp.concatenate([k[0, :, cols] for k in (k0, k1, k2, k3)], axis=0)
        values = jnp.concatenate([v[0, :, cols] for v in (v0, v1, v2, v3)], axis=0)
        for block, q in enumerate((q0, q1)):
            work.append((head, cols, block, mm(q[0, :, cols], keys, NT), values))
    for head, cols, block, products, values in work:
        scores = products * (SCALE * LOG2E) + bias
        peak = jnp.max(scores, axis=1, keepdims=True)
        powers = jnp.exp2(scores - peak)
        total = jnp.sum(powers, axis=1, keepdims=True)
        live = live_limit(sp, slot, block, (ROWS, 1), 0)
        inverse = jnp.where(live, 1.0 / total, 0.0)
        mixed = mm(powers.astype(jnp.bfloat16), values, NN) * inverse
        att[block, :, cols] = mixed.astype(jnp.bfloat16)
        level = jnp.where(live, peak + jnp.log2(total), -NEGATIVE)
        lse[head, :, block * ROWS : (block + 1) * ROWS] = jnp.broadcast_to(level, (ROWS, HD)).T[:8]


def bwd_kernel(
    slot, sp, q0, k0, v0, q1, k1, v1, k2, v2, k3, v3, att, lse, do0, do1, own, r1, r2, r3
):
    bias = key_bias(sp, slot, 0)
    low = jnp.bfloat16
    for head in range(TOGETHER_BACK):
        cols = slice(head * HD, (head + 1) * HD)
        keys = jnp.concatenate([k[0, :, cols] for k in (k0, k1, k2, k3)], axis=0)
        values = jnp.concatenate([v[0, :, cols] for v in (v0, v1, v2, v3)], axis=0)
        grad_k = None
        grad_v = None
        for block, (q, do) in enumerate(((q0, do0), (q1, do1))):
            q_rows = q[0, :, cols]
            d_rows = do[0, :, cols]
            scores = mm(keys, q_rows, NT) * (SCALE * LOG2E) + bias
            level = lse[head, 0:1, block * ROWS : (block + 1) * ROWS]
            probs = jnp.exp2(scores - level)
            product = d_rows.astype(jnp.float32) * att[block, :, cols].astype(jnp.float32)
            dots = jnp.sum(product.T, axis=0, keepdims=True)
            d_probs = mm(values, d_rows, NT)
            d_scores = (probs * (d_probs - dots)).astype(low)
            v_part = mm(probs.astype(low), d_rows, NN)
            k_part = mm(d_scores, q_rows, NN)
            grad_k = k_part if block == 0 else grad_k + k_part
            grad_v = v_part if block == 0 else grad_v + v_part
            grad_q = (mm(keys, d_scores, TN) * SCALE).T
            if block == 0:
                own[0, :, cols] = grad_q.astype(low)
            else:
                r1[0, :, cols] = grad_q.astype(low)
        grad_k = grad_k * SCALE
        own[1, :, cols] = grad_k[:ROWS].astype(low)
        own[2, :, cols] = grad_v[:ROWS].astype(low)
        r1[1, :, cols] = grad_k[ROWS : 2 * ROWS].astype(low)
        r1[2, :, cols] = grad_v[ROWS : 2 * ROWS].astype(low)
        r2[0, :, cols] = grad_k[2 * ROWS : 3 * ROWS].astype(low)
        r2[1, :, cols] = grad_v[2 * ROWS : 3 * ROWS].astype(low)
        r3[0, :, cols] = grad_k[3 * ROWS :].astype(low)
        r3[1, :, cols] = grad_v[3 * ROWS :].astype(low)


def head_block(lead, index=0, heads=1):
    return pl.BlockSpec((lead, ROWS, heads * HD), lambda h, sp: (index, 0, h))


def section_specs(slot, heads=1):
    def own(member):
        return pl.BlockSpec(
            (1, ROWS, heads * HD),
            lambda h, sp: (slot, 0, (12 * member + HEADS_HALF * sp[0, 0]) // heads + h),
        )

    return [own(0), own(1), own(2)] + [head_block(1, m, heads) for m in (0, 1, 2, 0, 1, 0, 1)]


def sections(qkv, x1, x2, x3):
    return (qkv, qkv, qkv, x1, x1, x1, x2, x2, x3, x3)


PAIRS = HEADS_HALF * 512 * 1024


def attend(sp, slot, qkv, received):
    return pl.pallas_call(
        functools.partial(fwd_kernel, slot),
        grid_spec=pltpu.PrefetchScalarGridSpec(
            num_scalar_prefetch=1,
            grid=(HEADS_HALF // TOGETHER,),
            in_specs=section_specs(slot, TOGETHER),
            out_specs=[
                head_block(2, 0, TOGETHER),
                pl.BlockSpec((TOGETHER, 8, 2 * ROWS), lambda h, sp: (h, 0, 0)),
            ],
        ),
        out_shape=[
            jax.ShapeDtypeStruct((2, ROWS, HALF), jnp.bfloat16),
            jax.ShapeDtypeStruct((HEADS_HALF, 8, 2 * ROWS), jnp.float32),
        ],
        cost_estimate=cost(4 * PAIRS * HD, 5e6, PAIRS),
    )(sp, *sections(qkv, *received))


def attend_back(sp, slot, qkv, received, att, lse, d_own, d_peer):
    heads = TOGETHER_BACK
    d_own_spec = pl.BlockSpec(
        (1, ROWS, heads * HD), lambda h, sp: (0, 0, HEADS_HALF // heads * sp[0, 0] + h)
    )

    def shape(count, kind):
        return jax.ShapeDtypeStruct((count, ROWS, HALF), kind)

    def piece(count):
        return head_block(count, 0, heads)

    return pl.pallas_call(
        functools.partial(bwd_kernel, slot),
        grid_spec=pltpu.PrefetchScalarGridSpec(
            num_scalar_prefetch=1,
            grid=(HEADS_HALF // heads,),
            in_specs=section_specs(slot, heads)
            + [
                piece(2),
                pl.BlockSpec((heads, 8, 2 * ROWS), lambda h, sp: (h, 0, 0)),
                d_own_spec,
                d_own_spec,
            ],
            out_specs=[piece(3), piece(3), piece(2), piece(2)],
        ),
        out_shape=[
            shape(3, jnp.bfloat16),
            shape(3, jnp.bfloat16),
            shape(2, jnp.bfloat16),
            shape(2, jnp.bfloat16),
        ],
        cost_estimate=cost(10 * PAIRS * HD, 1e7, PAIRS),
    )(sp, *sections(qkv, *received), att, lse, d_own, d_peer)


def join_kernel(sp, own, p1, p2, p3, *rest):
    out = rest[-1]
    core = sp[0, 0]
    member = pl.program_id(0)
    crossing = jnp.where(member > 0, 1.0, 0.0)
    mine = own[0].astype(jnp.float32) + crossing * p2[0].astype(jnp.float32)
    other = p1[0].astype(jnp.float32) + crossing * p3[0].astype(jnp.float32)
    first = core == 0
    out[0, :, :HALF] = jnp.where(first, mine, other).astype(jnp.bfloat16)
    out[0, :, HALF:] = jnp.where(first, other, mine).astype(jnp.bfloat16)


def join(sp, slot, own, p1, p2, p3, base):
    def piece(shift):
        return pl.BlockSpec((1, ROWS, HALF), lambda m, sp: (jnp.maximum(m - shift, 0), 0, 0))

    in_specs = [piece(0), piece(0), piece(1), piece(1)]
    args = [own, p1, p2, p3]
    aliases = {}
    if base is not None:
        in_specs.append(pl.BlockSpec(memory_space=pl.ANY))
        args.append(base)
        aliases = {5: 0}
    return pl.pallas_call(
        join_kernel,
        grid_spec=pltpu.PrefetchScalarGridSpec(
            num_scalar_prefetch=1,
            grid=(3,),
            in_specs=in_specs,
            out_specs=pl.BlockSpec((1, ROWS, WIDTH), lambda m, sp: (slot, 0, m)),
        ),
        out_shape=jax.ShapeDtypeStruct((2, ROWS, 3 * WIDTH), jnp.bfloat16),
        input_output_aliases=aliases,
        cost_estimate=cost(1e6, 1e7),
    )(sp, *args)


def pick_kernel(order, rows, out):
    def step(slot, carry):
        out[slot] = rows[order[slot]]
        return carry

    lax.fori_loop(0, rows.shape[0], step, 0)


def pick(rows, order):
    whole = pl.BlockSpec(rows.shape, lambda i, order: (0, 0, 0))
    return pl.pallas_call(
        pick_kernel,
        grid_spec=pltpu.PrefetchScalarGridSpec(
            num_scalar_prefetch=1, grid=(1,), in_specs=[whole], out_specs=whole
        ),
        out_shape=jax.ShapeDtypeStruct(rows.shape, rows.dtype),
        cost_estimate=cost(1e6, 2 * rows.size * 2),
    )(order, rows)


def rows_kernel(slot, sp, cotangent, gate, weight, send, keep, rows, total):
    step = pl.program_id(0)
    scaled = (cotangent[0].astype(jnp.float32) * gate[slot : slot + 1]).astype(jnp.bfloat16)

    @pl.when(step < 2)
    def _():
        send[...] = scaled

    @pl.when(step >= 2)
    def _():
        keep[...] = scaled

    product = mm(scaled, weight[...], NT)

    @pl.when(step == 0)
    def _():
        total[...] = product

    @pl.when((step > 0) & (step < 3))
    def _():
        total[...] += product

    @pl.when(step == 3)
    def _():
        rows[...] = (total[...] + product).astype(jnp.bfloat16)


def scaled_rows(sp, slot, cotangent, gate, out_weight):
    cols = D // 4

    def place(step, sp):
        core = sp[0, 0]
        return jnp.where(step < 2, 2 * (1 - core), 2 * core - 2) + step

    def shape(cols):
        return jax.ShapeDtypeStruct((ROWS, cols), jnp.bfloat16)

    return pl.pallas_call(
        functools.partial(rows_kernel, slot),
        grid_spec=pltpu.PrefetchScalarGridSpec(
            num_scalar_prefetch=1,
            grid=(4,),
            in_specs=[
                pl.BlockSpec((1, ROWS, cols), lambda k, sp: (slot, 0, place(k, sp))),
                pl.BlockSpec((2, cols), lambda k, sp: (0, place(k, sp))),
                pl.BlockSpec((WIDTH, cols), lambda k, sp: (0, place(k, sp))),
            ],
            out_specs=[
                pl.BlockSpec((ROWS, cols), lambda k, sp: (0, jnp.minimum(k, 1))),
                pl.BlockSpec((ROWS, cols), lambda k, sp: (0, jnp.maximum(k - 2, 0))),
                pl.BlockSpec((ROWS, WIDTH), lambda k, sp: (0, 0)),
            ],
            scratch_shapes=[pltpu.VMEM((ROWS, WIDTH), jnp.float32)],
        ),
        out_shape=[shape(D // 2), shape(D // 2), shape(WIDTH)],
        cost_estimate=cost(2 * 256 * WIDTH * D, 1.3e7),
    )(sp, cotangent, gate, out_weight)


def project_kernel(sp, a0, a1, b0, b1, w_mine, w_other, gate, cotangent, mixed, gate_grad):
    mine = jnp.concatenate([a0[0], a1[0]], axis=0)
    other = jnp.concatenate([b0[0], b1[0]], axis=0)
    outputs = mm(mine, w_mine[...], NN) + mm(other, w_other[...], NN)
    for slot in range(2):
        rows = outputs[slot * ROWS : (slot + 1) * ROWS]
        mixed[slot] = (rows * gate[slot : slot + 1]).astype(jnp.bfloat16)
        gate_grad[slot : slot + 1] = jnp.sum(
            cotangent[slot].astype(jnp.float32) * rows, axis=0, keepdims=True
        )


def project(sp, mine, other, out_weight, gate, cotangent):
    cols = 1024

    def rows(index):
        return pl.BlockSpec((1, ROWS, HALF), lambda d, sp: (index, 0, 0))

    wide = pl.BlockSpec((2, ROWS, cols), lambda d, sp: (0, 0, d))
    thin = pl.BlockSpec((2, cols), lambda d, sp: (0, d))
    return pl.pallas_call(
        project_kernel,
        grid_spec=pltpu.PrefetchScalarGridSpec(
            num_scalar_prefetch=1,
            grid=(D // cols,),
            in_specs=[
                rows(0),
                rows(0),
                rows(1),
                rows(1),
                pl.BlockSpec((HALF, cols), lambda d, sp: (sp[0, 0], d)),
                pl.BlockSpec((HALF, cols), lambda d, sp: (1 - sp[0, 0], d)),
                thin,
                wide,
            ],
            out_specs=[wide, thin],
        ),
        out_shape=[
            jax.ShapeDtypeStruct((2, ROWS, D), jnp.bfloat16),
            jax.ShapeDtypeStruct((2, D), jnp.float32),
        ],
        cost_estimate=cost(2 * 512 * WIDTH * D, 1.6e7),
    )(sp, mine[0], mine[1], other[0], other[1], out_weight, out_weight, gate, cotangent)


def weigh_kernel(sp, own0, peer0, own1, peer1, a0, a1, b0, b1, *rest):
    outs, product = rest[:8], rest[8]
    step = pl.program_id(0)
    left = jnp.concatenate([own0[...], peer0[...], own1[...], peer1[...]], axis=0)
    mine = jnp.concatenate([a0[0], a0[1], a1[0], a1[1]], axis=0)
    other = jnp.concatenate([b0[1], b0[0], b1[1], b1[0]], axis=0)
    by_x = mm(left, mine, TN).astype(jnp.bfloat16)
    for x_step in range(4):

        @pl.when(step == x_step)
        def _():
            outs[x_step][...] = by_x

    product[...] = mm(left, other, TN)
    for y_step in range(4):
        start = pl.multiple_of((sp[1, 5] ^ y_step) * SHARE, 8)
        rows = product[pl.ds(start, SHARE), :].astype(jnp.bfloat16)
        outs[4 + y_step][sp[0, 5] ^ step] = rows


def weigh(sp, scaled, mine, other):
    rows = D // 8
    pair = pl.BlockSpec((2, ROWS, HALF), lambda d, sp: (0, 0, 0))
    wide = pl.BlockSpec((ROWS, rows), lambda d, sp: (0, sp[0, 5] ^ d))
    return pl.pallas_call(
        weigh_kernel,
        grid_spec=pltpu.PrefetchScalarGridSpec(
            num_scalar_prefetch=1,
            grid=(4,),
            in_specs=[wide] * 4 + [pair] * 4,
            out_specs=[pl.BlockSpec((rows, HALF), lambda d, sp: (0, 0))] * 4
            + [pl.BlockSpec((4, SHARE, HALF), lambda d, sp: (0, 0, 0))] * 4,
            scratch_shapes=[pltpu.VMEM((rows, HALF), jnp.float32)],
        ),
        out_shape=[jax.ShapeDtypeStruct((rows, HALF), jnp.bfloat16)] * 4
        + [jax.ShapeDtypeStruct((4, SHARE, HALF), jnp.bfloat16)] * 4,
        cost_estimate=cost(2 * 1024 * WIDTH * D // 2, 1.2e7),
    )(sp, *scaled, mine[0], mine[1], other[0], other[1])


def along_x(x, step):
    return lax.ppermute(x, "dp", [(g, g ^ (step << 3)) for g in range(32)])


def along_y(x, step):
    return lax.ppermute(x, "dp", [(g, g ^ (step << 1)) for g in range(32)])


def add_up(refs):
    total = refs[0][...].astype(jnp.float32)
    for ref in refs[1:]:
        total = total + ref[...].astype(jnp.float32)
    return total


def part_kernel(sp, *refs):
    by_x, by_y, outs, total = refs[:4], refs[4:8], refs[8:16], refs[16]
    total[...] = add_up(by_x)
    for step in range(4):
        start = pl.multiple_of((sp[1, 5] ^ step) * SHARE, 8)
        outs[step][...] = total[pl.ds(start, SHARE), :].astype(jnp.bfloat16)
    for step in range(4):
        place = sp[0, 5] ^ step
        rows = by_y[0][place].astype(jnp.float32)
        for ref in by_y[1:]:
            rows = rows + ref[place].astype(jnp.float32)
        outs[4 + step][...] = rows.astype(jnp.bfloat16)


def sum_parts(sp, by_x, by_y):
    cols = HALF // 2
    share = pl.BlockSpec((SHARE, cols), lambda i, sp: (0, i))
    return pl.pallas_call(
        part_kernel,
        grid_spec=pltpu.PrefetchScalarGridSpec(
            num_scalar_prefetch=1,
            grid=(2,),
            in_specs=[pl.BlockSpec((4 * SHARE, cols), lambda i, sp: (0, i))] * 4
            + [pl.BlockSpec((4, SHARE, cols), lambda i, sp: (0, 0, i))] * 4,
            out_specs=[share] * 8,
            scratch_shapes=[pltpu.VMEM((4 * SHARE, cols), jnp.float32)],
        ),
        out_shape=[jax.ShapeDtypeStruct((SHARE, HALF), jnp.bfloat16)] * 8,
        cost_estimate=cost(5e6, 6e6),
    )(sp, *by_x, *by_y)


def final_moves(step):
    moves = []
    for xy in range(16):
        for z_low in range(2):
            for z_high in range(2):
                for core in range(2):
                    source = 4 * (2 * xy + z_low) + 2 * z_high + core
                    target = 4 * (16 * core + xy) + ((2 * z_low + z_high) ^ step)
                    moves.append((source, target))
    return moves


def sum_kernel(sp, *refs):
    low, high, outs, total = refs[:4], refs[4:8], refs[8:12], refs[12]
    first = sp[0, 0] == 0
    mine = add_up(low)
    other = add_up(high)
    total[:, :HALF] = jnp.where(first, mine, other)
    total[:, HALF:] = jnp.where(first, other, mine)
    count = SHARE // 4
    for step, out in enumerate(outs):
        start = pl.multiple_of((sp[1, 0] ^ step) * count, 8)
        out[...] = total[pl.ds(start, count), :].astype(jnp.bfloat16)


def sum_weights(sp, low, high):
    def whole(rows, cols):
        return pl.BlockSpec((rows, cols), lambda i, sp: (0, 0))

    return pl.pallas_call(
        sum_kernel,
        grid_spec=pltpu.PrefetchScalarGridSpec(
            num_scalar_prefetch=1,
            grid=(1,),
            in_specs=[whole(SHARE, HALF)] * 8,
            out_specs=[whole(SHARE // 4, WIDTH)] * 4,
            scratch_shapes=[pltpu.VMEM((SHARE, WIDTH), jnp.float32)],
        ),
        out_shape=[jax.ShapeDtypeStruct((SHARE // 4, WIDTH), jnp.bfloat16)] * 4,
        cost_estimate=cost(1e6, 2e6),
    )(sp, *low, *high)


def finish_weights(quarters):
    pieces = [
        lax.ppermute(quarter, ("dp", "seq"), final_moves(step)).astype(jnp.float32)
        for step, quarter in enumerate(quarters)
    ]
    return (pieces[0] + pieces[1] + pieces[2] + pieces[3]).T


def after(value, *others):
    return lax.optimization_barrier((value, *others))[0]


def spread_out(rows):
    groups = lax.axis_size("dp")
    portions = rows.reshape(groups, -1, rows.shape[-1])
    return lax.all_to_all(portions, "dp", split_axis=0, concat_axis=0, tiled=True)


def land(arranged, shape):
    landed = lax.all_to_all(arranged, "dp", split_axis=0, concat_axis=0, tiled=True)
    return landed.reshape(shape)


def body(qkv, gate, cotangent, out_weight, clip_lengths, text_lengths, plan):
    groups = lax.axis_size("dp")
    group_index = lax.axis_index("dp")
    seq_index = lax.axis_index("seq")
    core = seq_index & 1
    z_place = 2 * (group_index & 1) + (seq_index >> 1)
    ordinal = jnp.arange(groups, dtype=jnp.int32)
    inverse = jnp.sum(jnp.where(plan[None, :] == ordinal[:, None], ordinal[None, :], 0), axis=1)

    quarters = seq_index ^ jnp.arange(4, dtype=jnp.int32)
    text = lax.dynamic_slice_in_dim(text_lengths, 2 * group_index, 2)[:, None]
    video = lax.dynamic_slice_in_dim(clip_lengths, 2 * group_index, 2)[:, None]
    limits = jnp.where(quarters[None] == 0, text, video - (quarters[None] - 1) * ROWS)
    place = jnp.stack([core, z_place]).astype(jnp.int32)[:, None]
    plane = jnp.stack([group_index >> 3, (group_index >> 1) & 3]).astype(jnp.int32)[:, None]
    sp = jnp.concatenate([place, limits.astype(jnp.int32), plane], axis=1)

    def to_core(rows):
        return swap(rows[None], 1)

    received = [None, None]
    d_own, d_peer = [None, None], [None, None]
    att, lse = [None, None], [None, None]

    cp = core.astype(jnp.int32).reshape(1, 1)
    s1, s2, s3 = prep(cp, qkv, 1)
    near_keys = (swap(s1, 1), swap(s3, 3))
    received[1] = (near_keys[0], swap(s2, 2), near_keys[1])
    send_1, keep_1, away = scaled_rows(after(cp, s2), 1, cotangent, gate, out_weight)
    d_spread = spread_out(away)
    send_0, keep_0, near = scaled_rows(after(cp, away), 0, cotangent, gate, out_weight)
    d_own[0], d_peer[0] = near[None], to_core(near)
    scaled = (keep_0, swap(send_0, 1), keep_1, swap(send_1, 1))
    d_picked = pick(d_spread, after(plan, near, sp))
    landed = land(d_picked, (ROWS, WIDTH))
    s1, s2, s3 = prep(after(cp, d_picked), qkv, 0)
    near_keys = (swap(s1, 1), swap(s3, 3))
    received[0] = (near_keys[0], swap(s2, 2), near_keys[1])
    sp = after(sp, s2)
    att[1], lse[1] = attend(sp, 1, qkv, received[1])
    d_own[1], d_peer[1] = landed[None], to_core(landed)
    att_spread = spread_out(after(att[1], landed).reshape(2 * ROWS, HALF))

    def back(sp, slot):
        return attend_back(
            sp, slot, qkv, received[slot], att[slot], lse[slot], d_own[slot], d_peer[slot]
        )

    own_1, r1, r2, r3 = back(sp, 1)
    picked = pick(att_spread, after(inverse, r2))
    moved = land(picked, (2, ROWS, HALF))
    pieces_1 = (swap(r1, 1), swap(r2, 2), swap(r3, 3))
    att[0], lse[0] = attend(after(sp, picked), 0, qkv, received[0])
    att_other = [swap(att[0], 1)]
    own_0, *sent_0 = back(after(sp, lse[0]), 0)
    pieces_0 = [swap(rows, 1 + i) for i, rows in enumerate(sent_0)]
    balanced = [att[0], moved]
    att_other.append(swap(moved, 1))
    *partial, = weigh(after(sp, sent_0[1]), scaled, balanced, att_other)
    by_x, by_y = partial[:4], partial[4:]
    for step in (2, 1, 3):
        by_x[step] = along_x(by_x[step], step)
        by_y[step] = along_y(by_y[step], step)
    mixed, gate_part = project(
        after(sp, partial[0]), balanced, att_other, out_weight, gate, cotangent
    )
    gate_grad = gate_part + swap(gate_part, 1) + swap(gate_part, 2) + swap(gate_part, 3)
    grads = join(after(sp, gate_part), 1, own_1, *pieces_1, None)
    parts = list(sum_parts(after(sp, grads), by_x, by_y))
    low = parts[:1] + [along_y(parts[step], step) for step in (1, 2, 3)]
    high = parts[4:5] + [along_x(parts[4 + step], step) for step in (1, 2, 3)]
    grads = join(after(sp, parts[0]), 0, own_0, *pieces_0, grads)
    quarters = sum_weights(after(sp, grads), low, high)
    weight_grad = finish_weights(quarters)
    return (mixed, gate_grad, weight_grad, grads)


def solution(mesh):
    in_specs = (P("dp", "seq", None), P("dp", None), P("dp", "seq", None), P(), P(), P(), P())
    out_specs = (P("dp", "seq", None), P("dp", None), P(None, ("dp", "seq")), P("dp", "seq", None))
    return jax.shard_map(body, mesh=mesh, in_specs=in_specs, out_specs=out_specs, check_vma=False)
```
